512 devices in a mesh: gx: 64 (over y_lo, z, core), gy: 8 (over x, y_hi).
Axes of the slice: x: 4, y: 8 (y_hi: 2, y_lo: 4; y = y_hi * 4 + y_lo), z: 8, core: 2. Of those that a mesh axis runs over, the one named last changes fastest.
Arguments:
- charge_density: float32 [16, 32, 128, 1024], P(None, None, 'gx', 'gy'), may hold values from -48 to 48
- layer_ids: int32 [32, 128, 1024], P(None, 'gx', 'gy'), may hold values from 0 to 7
- eps_mean: float32 [8], replicated, may hold values from 1 to 4
- eps_fluct: float32 [8, 15], replicated, may hold values from -0.5 to 0.5
- galerkin: float32 [16, 16, 16], replicated, may hold values from -0.5 to 1, as said below
- net_ids: int32 [32, 128, 8], P(None, 'gx', 'gy'), may hold values from 0 to 2047
- net_place: int32 [2048], replicated, may hold values from 0 to 2047, each once
Outputs:
- potential: float32 [16, 32, 128, 1024], P(None, None, 'gx', 'gy')
- charges: float32 [16, 2048], P(None, ('gx', 'gy'))
The draws below stay inside these ranges and needn't reach their ends.
Inputs may be any that keep to these rules, and one draw needn't show every extreme that they name: `galerkin`: G[0] is the identity; every G[i] is symmetric in j and k; for i >= 1 its diagonal lies within -0.1 to 0.1.
All inputs are finite; a program needn't handle non-finite values.
Results may differ from the reference program's by a relative error of at most 0.0001.
Values sent between devices are 32-bit elements; how exact they have to be, the bound alone decides.
A program may use at most 64 MiB of HBM per device.

```python
import math
import jax
import jax.numpy as jnp
from jax import lax

MODES = 16
LAYERS = 8
NZ = 32
CY = 128
ITERS = 2
NX = 128
NY = 1024
NETS = 2048
N_GY = 8


def draw_galerkin(key, part):
    first, second = jax.random.split(jax.random.fold_in(key, 11))
    offdiag = jax.random.uniform(first, (MODES - 1, MODES, MODES), jnp.float32, -0.5, 0.5)
    symmetric = 0.5 * (offdiag + jnp.transpose(offdiag, (0, 2, 1)))
    diagonal = jax.random.uniform(second, (MODES - 1, MODES), jnp.float32, -0.1, 0.1)
    identity = jnp.eye(MODES, dtype=jnp.float32)
    others = symmetric * (1.0 - identity) + diagonal[:, :, None] * identity
    return jnp.concatenate([identity[None], others], 0).astype(jnp.float32)


def touch_ends(drawn, rng, low, largest):
    spot = [jax.random.randint(jax.random.fold_in(rng, axis), (), 0, length) for axis, length in enumerate(drawn.shape)]
    longest = drawn.shape.index(max(drawn.shape))
    neighbour = spot[:longest] + [(spot[longest] + 1) % drawn.shape[longest]] + spot[longest + 1:]
    return drawn.at[tuple(spot)].set(low).at[tuple(neighbour)].set(largest)


def levels(stream_key, extent, pieces, smallest, largest):
    def one(axis_at, parts):
        heights = jax.random.uniform(jax.random.fold_in(jax.random.fold_in(stream_key, 6), axis_at), (parts,), jnp.float32, smallest / len(pieces), largest / len(pieces))
        return jnp.repeat(jnp.exp(heights), extent[axis_at] // parts).reshape((-1,) + (1,) * (len(extent) - axis_at - 1))

    loudness = one(*pieces[0])
    for cut in pieces[1:]:
        loudness = loudness * one(*cut)
    return loudness


def normal_values(own_key, extent, deviation, bound, cuts=(), kind=jnp.bfloat16):
    values = jax.random.normal(own_key, extent, jnp.float32) * deviation
    if len(cuts) > 0:
        values = levels(own_key, extent, cuts, -0.22, 0.18) * values
    return jnp.clip(values, min=-bound, max=bound).astype(kind)


def setup_inputs(seed: int = 0) -> dict:
    arg_keys = jax.random.split(jax.random.key(seed), 8)
    return {
        "charge_density": normal_values(arg_keys[0], (MODES, NZ, NX, NY), 8.0, 48.0, ((2, 64), (3, 8)), jnp.float32),
        "layer_ids": touch_ends(jax.random.randint(arg_keys[1], (NZ, NX, NY), 0, LAYERS), jax.random.fold_in(arg_keys[1], 1), 0, LAYERS - 1).astype(jnp.int32),
        "eps_mean": jnp.clip(jnp.exp(jax.random.uniform(arg_keys[2], (LAYERS,), jnp.float32, math.log(1.0), math.log(4.0))), 1.0, 4.0),
        "eps_fluct": jnp.clip(jax.random.uniform(arg_keys[3], (LAYERS, MODES - 1), jnp.float32, -0.5, 0.5), -0.5, 0.5),
        "galerkin": draw_galerkin(jax.random.fold_in(arg_keys[7], 71), 0),
        "net_ids": touch_ends(jax.random.randint(arg_keys[5], (NZ, NX, N_GY), 0, NETS), jax.random.fold_in(arg_keys[5], 1), 0, NETS - 1).astype(jnp.int32),
        "net_place": jax.random.permutation(arg_keys[6], NETS).astype(jnp.int32),
    }


charge_scale = 1.0 / 512.0
relax = 0.8


def neighbours(field):
    padded = jnp.pad(field, ((0, 0), (1, 1), (1, 1), (1, 1)))
    total = padded[:, 2:, 1:-1, 1:-1] + padded[:, :-2, 1:-1, 1:-1]
    total = total + padded[:, 1:-1, 2:, 1:-1] + padded[:, 1:-1, :-2, 1:-1]
    return total + padded[:, 1:-1, 1:-1, 2:] + padded[:, 1:-1, 1:-1, :-2]


def contract_flat(gflat, coeffs, field):
    modes = coeffs.shape[0]
    product = (coeffs[:, None, :] * field[None, :, :]).reshape(modes * modes, coeffs.shape[1])
    return jnp.dot(gflat, product, precision=lax.Precision.HIGHEST, preferred_element_type=jnp.float32)


def contract(gflat, coeffs, field):
    modes = coeffs.shape[0]
    shape = coeffs.shape
    coeff_z = jnp.moveaxis(coeffs, 1, 0).reshape(shape[1], modes, -1)
    field_z = jnp.moveaxis(field, 1, 0).reshape(shape[1], modes, -1)
    result = lax.map(lambda pair: contract_flat(gflat, pair[0], pair[1]), (coeff_z, field_z))
    return jnp.moveaxis(result.reshape(shape[1], modes, shape[2], shape[3]), 0, 1)


def reference(charge_density, layer_ids, eps_mean, eps_fluct, galerkin, net_ids, net_place):
    modes = galerkin.shape[0]
    layers = eps_mean.shape[0]
    table = jnp.concatenate([eps_mean[None, :], eps_mean[None, :] * eps_fluct.T], 0)
    onehot = (layer_ids[None] == jnp.arange(layers, dtype=jnp.int32)[:, None, None, None]).astype(jnp.float32)
    permit = jnp.einsum("il,lzxy->izxy", table, onehot, precision=lax.Precision.HIGHEST)
    weights = 6.0 * permit + neighbours(permit)
    gdiag = jnp.diagonal(galerkin, axis1=1, axis2=2)
    diag = 0.5 * jnp.einsum("ik,izxy->kzxy", gdiag, weights, precision=lax.Precision.HIGHEST)
    gflat = jnp.transpose(galerkin, (2, 0, 1)).reshape(modes, modes * modes)

    def operate(field):
        weighted = contract(gflat, permit, field)
        return 0.5 * (contract(gflat, weights, field) - contract(gflat, permit, neighbours(field)) - neighbours(weighted))

    potential = relax * charge_density / diag
    for iteration in range(ITERS - 1):
        potential = potential + relax * (charge_density - operate(potential)) / diag
    flux = operate(potential)
    shape = flux.shape
    blocksum = flux.reshape(modes, shape[1], shape[2], shape[3] // CY, CY).sum(-1).reshape(modes, -1)
    column = net_place[net_ids.reshape(-1)]
    nets = net_place.shape[0]
    charges = jax.ops.segment_sum(blocksum.T, column, num_segments=nets).T * charge_scale
    return potential, charges
```

```python
import functools

import jax
import jax.numpy as jnp
from jax import lax
from jax.experimental import pallas as pl
from jax.experimental.pallas import tpu as pltpu
from jax.sharding import PartitionSpec as P

charge_scale = 1.0 / 512.0
relax = 0.8

Y_LO, SZ, CORES = 4, 8, 2
SX, Y_HI = 4, 2
MODES, LAYERS = 16, 8
NZ, ROWS, LANES = 32, 64, 128
CHUNK = 8
MESH = pl.DeviceIdType.MESH
F32, BF16, I32 = jnp.float32, jnp.bfloat16, jnp.int32

BESIDE = ((-1, 0), (1, 0), (0, -1), (0, 1), (-1, -1), (-1, 1), (1, -1), (1, 1))
SLOT = {offset: q for q, offset in enumerate(BESIDE)}


def lanes(shape):
    return lax.broadcasted_iota(I32, shape, len(shape) - 1)


def rows(shape):
    return lax.broadcasted_iota(I32, shape, 0)


def packed(ids):
    return jnp.where(ids < LAYERS, jnp.left_shift(1, (ids & 7) * 4), 0)


def counts(word):
    out = []
    for l in range(LAYERS):
        one = (lax.shift_right_logical(word, 4 * l) & 15).astype(F32)
        out.append(jnp.concatenate([one, one], 0))
    return out


def wide(ref, r):
    return jnp.broadcast_to(ref[pl.ds(r, 1), :], (8, LANES))


def bits(ids):
    two = jnp.concatenate([ids, ids], 0)
    return [(two & (1 << b)) != 0 for b in range(3)]


def pick(mask, parts):
    for m in mask:
        parts = [jnp.where(m, parts[i + 1], parts[i]) for i in range(0, len(parts), 2)]
    return parts[0]


def weigh(cnt, parts):
    total = cnt[0] * parts[0]
    for c, part in zip(cnt[1:], parts[1:]):
        total = total + c * part
    return total


def apply_all(b3, tiles):
    high = [t.astype(BF16) for t in tiles]
    low = [(t - h.astype(F32)).astype(BF16) for t, h in zip(tiles, high)]
    high = jnp.concatenate(high, 1)
    rhs = jnp.concatenate([high, high, jnp.concatenate(low, 1)], 0)
    u = jnp.dot(b3, rhs, preferred_element_type=F32)
    return [
        [u[l * MODES : (l + 1) * MODES, i * LANES : (i + 1) * LANES] for l in range(LAYERS)]
        for i in range(len(tiles))
    ]


def kernel(
    gx_size, gy_size,
    rho_ref, ids_ref, mean_ref, fluct_ref, g_ref, net_ref, place_ref,
    pot_ref, charge_ref,
    rv, v, w, t, rd, hx, hv, hw, hid, ie, ier, es, er,
    b3_ref, d_ref, idh_ref, cw_ref, chw_ref, c4_ref, oht, s1, r1, s2, r2,
    ie_s, ie_r, hid_s, hid_r, hx_s, hx_r, e_s, e_r, r1_s, r1_r, r2_s, r2_r,
):
    gx, gy = lax.axis_index("gx"), lax.axis_index("gy")
    core, z, y_lo = gx % CORES, (gx // CORES) % SZ, gx // (CORES * SZ)
    x, y_hi = gy // Y_HI, gy % Y_HI
    g1, m_count = SZ * SX, Y_LO * CORES * Y_HI
    group = z * SX + x
    member = (y_lo * CORES + core) * Y_HI + y_hi

    def group_peer(s):
        peer = (group + s) % g1
        return ((y_lo * SZ + peer // SX) * CORES + core, (peer % SX) * Y_HI + y_hi), peer

    def member_peer(s):
        peer = (member + s) % m_count
        lo, c, hi = peer // (CORES * Y_HI), (peer // Y_HI) % CORES, peer % Y_HI
        return ((lo * SZ + z) * CORES + c, x * Y_HI + hi)

    def exists(q):
        dx, dy = BESIDE[q]
        ok = None
        for step, at, size in ((dx, gx, gx_size), (dy, gy, gy_size)):
            if step:
                here = at > 0 if step < 0 else at < size - 1
                ok = here if ok is None else jnp.logical_and(ok, here)
        return ok

    def target(q):
        return (gx + BESIDE[q][0], gy + BESIDE[q][1])

    def back(q):
        return SLOT[(-BESIDE[q][0], -BESIDE[q][1])]

    barrier = pltpu.get_barrier_semaphore()
    expected = g1 - 1 + m_count - 1
    for q in range(8):
        expected = expected + exists(q).astype(I32)

        @pl.when(exists(q))
        def _(q=q):
            pl.semaphore_signal(barrier, inc=1, device_id=target(q), device_id_type=MESH)

    @pl.loop(1, g1)
    def _(s):
        pl.semaphore_signal(barrier, inc=1, device_id=group_peer(s)[0], device_id_type=MESH)

    @pl.loop(1, m_count)
    def _(s):
        pl.semaphore_signal(barrier, inc=1, device_id=member_peer(s), device_id_type=MESH)

    lane16 = lanes((MODES, LANES))
    lane1 = lanes((1, LANES))
    lane64, row64 = lanes((ROWS, LANES)), rows((ROWS, LANES))
    on_low = lane64 == 2 * row64
    on_high = lane64 == ((2 * row64 + 127) & 127)

    own_ids = ids_ref[...]
    ids_f = own_ids.astype(F32)

    def edge_of(low, high):
        both = jnp.where(on_low, low, 0.0) + jnp.where(on_high, high, 0.0)
        return jnp.sum(both, axis=0, keepdims=True).astype(I32)

    net_f = net_ref[...].astype(F32)
    ie[...] = jnp.zeros((8, LANES), I32)
    ie[0:1, :] = edge_of(ids_f[:, 0:1], ids_f[:, 127:128])
    ie[1:2, :] = edge_of(ids_f[:, 1:2], ids_f[:, 126:127])
    ie[2:3, :] = edge_of(net_f, net_f)

    def gather_edge(tile, r, acc):
        mine = jnp.logical_or(lane16 == 2 * r, lane16 == ((2 * r + 127) & 127))
        return jnp.where(mine, pltpu.roll(tile, 2 * r, 1), acc)

    def rearrange(c, acc):
        for i in range(CHUNK):
            r = c * CHUNK + i
            tile = rho_ref[pl.ds(r, MODES, stride=ROWS), :]
            rv[c * (CHUNK // 2) + i // 2, i % 2] = tile
            acc = gather_edge(tile, r, acc)
        return acc

    es[...] = lax.fori_loop(0, ROWS // CHUNK, rearrange, jnp.zeros((MODES, LANES), F32))

    pl.semaphore_wait(barrier, expected)

    def rv_x(q):
        return rv.at[:, q]

    def ie_copy(q):
        return pltpu.make_async_remote_copy(
            ie, ier.at[back(q)], ie_s.at[q], ie_r.at[back(q)], device_id=target(q), device_id_type=MESH
        )

    def hid_copy(q):
        return pltpu.make_async_remote_copy(
            ids_ref, hid.at[back(q)], hid_s.at[q], hid_r.at[back(q)], device_id=target(q), device_id_type=MESH
        )

    def hx_copy(q):
        return pltpu.make_async_remote_copy(
            rv_x(q),
            hx.at[back(q)], hx_s.at[q], hx_r.at[back(q)], device_id=target(q), device_id_type=MESH,
        )

    def e_copy(q):
        return pltpu.make_async_remote_copy(
            es, er.at[back(q) - 2], e_s.at[q - 2], e_r.at[back(q) - 2], device_id=target(q), device_id_type=MESH
        )

    def copies(q):
        found = [ie_copy(q)]
        if q < 2:
            found += [hid_copy(q), hx_copy(q)]
        elif q < 4:
            found += [e_copy(q)]
        return found

    for q in (4, 5, 6, 7, 2, 3, 0, 1):
        @pl.when(exists(q))
        def _(q=q):
            for one in copies(q):
                one.start()

        @pl.when(jnp.logical_not(exists(q)))
        def _(q=q):
            ier[q] = jnp.where(rows((8, LANES)) < 2, LAYERS, -1)
            if q < 2:
                hid[q] = jnp.full((ROWS, LANES), LAYERS, I32)
                hx[q] = jnp.zeros((NZ, MODES, LANES), F32)
            elif q < 4:
                er[q - 2] = jnp.zeros((MODES, LANES), F32)

    for l in range(LAYERS):
        total = g_ref[0]
        for i in range(1, MODES):
            total = total + fluct_ref[l, i - 1] * g_ref[i]
        total = mean_ref[l] * total
        eye = rows((MODES, MODES)) == lanes((MODES, MODES))
        d_ref[l] = jnp.broadcast_to(
            jnp.sum(jnp.where(eye, total, 0.0), axis=1, keepdims=True), (MODES, LANES)
        )
        three = jnp.concatenate([total, total, total], 1)
        high = three.astype(BF16)
        low = (three - high.astype(F32)).astype(BF16).astype(F32)
        at = lanes((MODES, 3 * MODES))
        middle = jnp.logical_and(at >= MODES, at < 2 * MODES)
        b3_ref[pl.ds(l * MODES, MODES), :] = jnp.where(middle, low, high.astype(F32)).astype(BF16)

    zero = jnp.zeros((2, MODES, LANES), F32)
    for ref in (v, w):
        ref[0:2] = zero
        ref[ROWS + 2 : ROWS + 4] = zero

    def wait_recv(q, which):
        @pl.when(exists(q))
        def _():
            pltpu.make_async_remote_copy(
                *which(q), device_id=target(q), device_id_type=MESH
            ).wait_recv()

    for q in range(8):
        wait_recv(q, lambda q: (ie, ier.at[q], ie_s.at[q], ie_r.at[q]))
    for q in range(2):
        wait_recv(q, lambda q: (ids_ref, hid.at[q], hid_s.at[q], hid_r.at[q]))

    even64 = (row64 & 1) == 0
    left, right = hid[0], hid[1]

    def row_swap(low, high):
        return jnp.where(even64, pltpu.roll(low, ROWS - 1, 0), pltpu.roll(high, 1, 0))

    halo_ids = row_swap(left, right)
    outer_ids = jnp.where(even64, left, right)
    idh_ref[...] = halo_ids

    def roll1(row, by):
        return pltpu.roll(jnp.broadcast_to(row, (8, LANES)), by % LANES, 1)[0:1]

    quarter = lane1 & 3

    def beside_row(k):
        from_left, from_right = ier[2][k : k + 1], ier[3][k : k + 1]
        return jnp.where((lane1 & 1) == 0, roll1(from_left, 1), roll1(from_right, -1))

    edge_ids, edge_ids2 = beside_row(0), beside_row(1)
    ll, lr, rl, rr = (ier[q][0:1] for q in (4, 5, 6, 7))
    edge_halo = jnp.where(
        quarter == 0, roll1(ll, -1),
        jnp.where(quarter == 2, roll1(rl, 3), jnp.where(quarter == 3, roll1(lr, -3), roll1(rr, 1))),
    )
    own_edge = ie[0:1, :]

    def to_column(row, mask):
        return jnp.sum(jnp.where(mask, row.astype(F32), 0.0), axis=1, keepdims=True).astype(I32)

    def around_y(p, edge_row):
        word = packed(edge_row)
        low = jnp.bitwise_and(word, 0xFFFF)
        high = lax.shift_right_logical(word, 16)

        def column(mask):
            return to_column(low, mask) + jnp.left_shift(to_column(high, mask), 16)

        below = jnp.where(lane64 == 0, column(on_low), pltpu.roll(p, 1, 1))
        above = jnp.where(lane64 == LANES - 1, column(on_high), pltpu.roll(p, LANES - 1, 1))
        return below + above

    def around_z(p):
        up = jnp.where(row64 < ROWS - 2, pltpu.roll(p, ROWS - 2, 0), 0)
        return up + jnp.where(row64 >= 2, pltpu.roll(p, 2, 0), 0)

    p_own, p_halo = packed(own_ids), packed(halo_ids)
    four = around_z(p_own) + row_swap(p_own, p_own) + p_halo
    c4_ref[...] = four + 4 * p_own
    cw_ref[...] = four + around_y(p_own, edge_ids) + 6 * p_own
    chw_ref[...] = (
        around_z(p_halo) + p_own + packed(outer_ids) + around_y(p_halo, edge_halo) + 6 * p_halo
    )

    edge_z = lax.shift_right_logical((lane1 + 1) & (LANES - 1), 2)
    p_edge = packed(edge_ids)
    edge_low_x = jnp.logical_or(quarter == 0, quarter == 3)
    edge_word = (
        jnp.where(edge_z > 0, roll1(p_edge, 4), 0)
        + jnp.where(edge_z < NZ - 1, roll1(p_edge, -4), 0)
        + jnp.where(edge_low_x, roll1(p_edge, -2), roll1(p_edge, 2))
        + packed(edge_halo) + packed(own_edge) + packed(edge_ids2) + 6 * p_edge
    )

    b3 = b3_ref[...]

    def start(rho, word):
        cnt = counts(word)
        inverse = (2.0 * relax) / weigh(cnt, [d_ref[l] for l in range(LAYERS)])
        return rho * inverse, inverse, cnt

    @pl.loop(0, ROWS // CHUNK)
    def _(c):
        tiles, cnts = [], []
        for i in range(CHUNK):
            r = c * CHUNK + i
            tile, inverse, cnt = start(rv[c * (CHUNK // 2) + i // 2, i % 2], wide(cw_ref, r))
            rd[r] = inverse
            v[r + 2] = tile
            tiles.append(tile)
            cnts.append(cnt)
        u = apply_all(b3, tiles)
        for i in range(CHUNK):
            r = c * CHUNK + i
            w[r + 2] = pick(bits(wide(ids_ref, r)), u[i])
            t[r] = weigh(cnts[i], u[i])

    net_own = ie[2:3, :]
    odd_from = jnp.where(quarter == 3, roll1(ier[0][2:3], -2), roll1(ier[1][2:3], 2))
    nets = (
        jnp.where((lane1 & 1) == 0, net_own, odd_from),
        jnp.where((lane1 & 1) == 0, ier[2][2:3], ier[3][2:3]),
        net_own,
    )
    place = place_ref[...]
    place_parts = jnp.concatenate(
        [lax.shift_right_logical(place, 3).astype(F32), (place & 7).astype(F32)], 0
    ).astype(BF16)
    hi_rows = place.shape[0]
    columns = []
    for net in nets:
        chosen = (rows((LANES, LANES)) == (net & (LANES - 1))).astype(F32).astype(BF16)
        found = jnp.dot(place_parts, chosen, preferred_element_type=F32)
        value = 8.0 * found[:hi_rows] + found[hi_rows:]
        own_row = rows((hi_rows, LANES)) == lax.shift_right_logical(net, 7)
        column = jnp.sum(jnp.where(own_row, value, 0.0), axis=0, keepdims=True)
        columns.append(jnp.where(net < 0, -1.0, column).astype(I32))

    spot = rows((LANES, LANES))
    spot_m, spot_g, spot_c = spot // 8, (spot // 4) & 1, spot & 3
    per_gx = gy_size * 4
    spot_p = (
        ((spot_m // (CORES * Y_HI)) * SZ * CORES + (spot_m // Y_HI) % CORES) * per_gx
        + (spot_g * Y_HI + spot_m % Y_HI) * 4 + spot_c
    )
    spot_p = jnp.where(spot_m < m_count, spot_p, -2)

    @pl.loop(0, g1 // 2)
    def _(pair):
        base = (2 * pair // SX) * CORES * per_gx + ((2 * pair) % SX) * Y_HI * 4
        for b, column in enumerate(columns):
            hit = spot_p == column - base
            hit = jnp.logical_and(hit, spot_p >= 0)
            oht[pl.ds(pl.multiple_of(pair * LANES, LANES), LANES), b * LANES : (b + 1) * LANES] = (
                jnp.where(hit, 1.0, 0.0).astype(BF16)
            )

    for q in range(2):
        wait_recv(q, lambda q: (rv_x(q), hx.at[q], hx_s.at[q], hx_r.at[q]))

    @pl.loop(0, ROWS // CHUNK)
    def _(c):
        tiles = []
        for i in range(CHUNK):
            r = c * CHUNK + i
            tile, _, _ = start(hx[i % 2, c * (CHUNK // 2) + i // 2], wide(chw_ref, r))
            hv[r] = tile
            tiles.append(tile)
        u = apply_all(b3, tiles)
        for i in range(CHUNK):
            r = c * CHUNK + i
            hw[r] = pick(bits(wide(idh_ref, r)), u[i])

    for q in range(2, 4):
        wait_recv(q, lambda q: (es, er.at[q - 2], e_s.at[q - 2], e_r.at[q - 2]))

    even16 = (lane16 & 1) == 0
    edge_rho = jnp.where(even16, pltpu.roll(er[0], 1, 1), pltpu.roll(er[1], LANES - 1, 1))
    edge_v, _, _ = start(edge_rho, jnp.broadcast_to(edge_word, (8, LANES)))
    edge_bits = bits(jnp.broadcast_to(edge_ids, (8, LANES)))
    edge_w = pick(edge_bits, apply_all(b3, [edge_v])[0])

    def beside_y(tile, edge, r):
        mine = pltpu.roll(edge, (LANES - 2 * r) & (LANES - 1), 1)
        below = jnp.where(lane16 == 0, mine, pltpu.roll(tile, 1, 1))
        return below + jnp.where(lane16 == LANES - 1, mine, pltpu.roll(tile, LANES - 1, 1))

    def within(ref, c, i):
        r = c * CHUNK + i
        return ref[r] + ref[r + 4] + ref[c * CHUNK + (i ^ 1) + 2]

    @pl.loop(0, ROWS // CHUNK)
    def _(c):
        tiles = []
        for i in range(CHUNK):
            r = c * CHUNK + i
            tiles.append(within(v, c, i) + hv[r] + beside_y(v[r + 2], edge_v, r))
        u = apply_all(b3, tiles)
        for i in range(CHUNK):
            r = c * CHUNK + i
            near = within(w, c, i) + hw[r] + beside_y(w[r + 2], edge_w, r)
            flux = 0.5 * (t[r] - pick(bits(wide(ids_ref, r)), u[i]) - near)
            result = v[r + 2] + rd[r] * (rv[c * (CHUNK // 2) + i // 2, i % 2] - flux)
            hv[r] = result
            pot_ref[pl.ds(r, MODES, stride=ROWS), :] = result

    @pl.loop(0, ROWS // CHUNK, init_carry=(jnp.zeros((MODES, LANES), F32),) * 2)
    def sums(c, carry):
        acc, edge = carry
        tiles = [hv[c * CHUNK + i] for i in range(CHUNK)]
        u = apply_all(b3, tiles)
        for i in range(CHUNK):
            r = c * CHUNK + i
            v[r + 2] = tiles[i]
            edge = gather_edge(tiles[i], r, edge)
            own = pick(bits(wide(ids_ref, r)), u[i])
            w[r + 2] = own
            t[r] = weigh(counts(wide(c4_ref, r)), u[i])
            out = own + pick(bits(wide(idh_ref, r)), u[i])
            total = -0.5 * jnp.sum(out, axis=1, keepdims=True)
            acc = jnp.where(lane16 == ((2 * r + 127) & 127), total, acc)
        return acc, edge

    acc, edge_p = sums

    @pl.loop(0, ROWS // CHUNK, init_carry=acc)
    def acc(c, acc):
        u = apply_all(b3, [within(v, c, i) for i in range(CHUNK)])
        for i in range(CHUNK):
            r = c * CHUNK + i
            flux = t[r] - pick(bits(wide(ids_ref, r)), u[i]) - within(w, c, i)
            total = 0.5 * jnp.sum(flux, axis=1, keepdims=True)
            acc = jnp.where(lane16 == 2 * r, total, acc)
        return acc

    u = apply_all(b3, [edge_p])[0]
    inside = jnp.broadcast_to(edge_ids, (MODES, LANES)) < LAYERS
    across = 0.5 * (
        pick(bits(jnp.broadcast_to(own_edge, (8, LANES))), u) + jnp.where(inside, pick(edge_bits, u), 0.0)
    )
    blocks = jnp.concatenate([acc, -across, across], 1) * charge_scale
    high = blocks.astype(BF16)
    low = (blocks - high.astype(F32)).astype(BF16)
    parts = jnp.concatenate([high, low], 0)

    alternate = (lanes((8, LANES)) & 4) == 0

    @pl.loop(0, g1 // 2)
    def _(pair):
        placed = lax.dot_general(
            parts, oht[pl.ds(pl.multiple_of(pair * LANES, LANES), LANES), :],
            (((1,), (1,)), ((), ())), preferred_element_type=F32,
        )
        a = placed[0:8] + placed[16:24]
        b = placed[8:16] + placed[24:32]
        s1[2 * pair] = jnp.where(alternate, a, pltpu.roll(b, 4, 1))
        s1[2 * pair + 1] = jnp.where(alternate, pltpu.roll(a, LANES - 4, 1), b)

    def r1_copy(s):
        device, peer = group_peer(s)
        return pltpu.make_async_remote_copy(
            s1.at[peer], r1.at[s], r1_s.at[s], r1_r.at[s], device_id=device, device_id_type=MESH
        )

    def r2_copy(s):
        return pltpu.make_async_remote_copy(
            s2, r2.at[s], r2_s.at[s], r2_r.at[s], device_id=member_peer(s), device_id_type=MESH
        )

    @pl.loop(1, g1)
    def _(s):
        r1_copy(s).start()

    @pl.loop(1, g1, init_carry=s1[group])
    def share(s, total):
        r1_copy(s).wait_recv()
        return total + r1[s]

    s2[...] = share

    @pl.loop(1, m_count)
    def _(s):
        r2_copy(s).start()

    @pl.loop(1, m_count, init_carry=share)
    def final(s, total):
        r2_copy(s).wait_recv()
        return total + r2[s]

    turned = pltpu.roll(final, (LANES - 8 * member) & (LANES - 1), 1)
    charge_ref[...] = turned

    @pl.loop(1, g1)
    def _(s):
        r1_copy(s).wait_send()

    @pl.loop(1, m_count)
    def _(s):
        r2_copy(s).wait_send()

    for q in range(8):
        @pl.when(exists(q))
        def _(q=q):
            for one in copies(q):
                one.wait_send()


def local(gx_size, gy_size, charge_density, layer_ids, eps_mean, eps_fluct, galerkin, net_ids, net_place):
    vmem = pl.BlockSpec(memory_space=pltpu.VMEM)
    smem = pl.BlockSpec(memory_space=pltpu.SMEM)
    g1, m_count = SZ * SX, Y_LO * CORES * Y_HI
    tile = (MODES, LANES)
    dma = pltpu.SemaphoreType.DMA
    potential, charges = pl.pallas_call(
        functools.partial(kernel, gx_size, gy_size),
        out_shape=(
            jax.ShapeDtypeStruct((MODES * ROWS, LANES), F32),
            jax.ShapeDtypeStruct((8, LANES), F32),
        ),
        in_specs=[vmem, vmem, smem, smem, vmem, vmem, vmem],
        out_specs=(vmem, vmem),
        scratch_shapes=[
            pltpu.VMEM((NZ, 2) + tile, F32),
            pltpu.VMEM((ROWS + 4,) + tile, F32),
            pltpu.VMEM((ROWS + 4,) + tile, F32),
            pltpu.VMEM((ROWS,) + tile, F32),
            pltpu.VMEM((ROWS,) + tile, F32),
            pltpu.VMEM((2, NZ) + tile, F32),
            pltpu.VMEM((ROWS,) + tile, F32),
            pltpu.VMEM((ROWS,) + tile, F32),
            pltpu.VMEM((2, ROWS, LANES), I32),
            pltpu.VMEM((8, LANES), I32),
            pltpu.VMEM((8, 8, LANES), I32),
            pltpu.VMEM(tile, F32),
            pltpu.VMEM((2,) + tile, F32),
            pltpu.VMEM((LAYERS * MODES, 3 * MODES), BF16),
            pltpu.VMEM((LAYERS,) + tile, F32),
            pltpu.VMEM((ROWS, LANES), I32),
            pltpu.VMEM((ROWS, LANES), I32),
            pltpu.VMEM((ROWS, LANES), I32),
            pltpu.VMEM((ROWS, LANES), I32),
            pltpu.VMEM((g1 // 2 * LANES, 3 * LANES), BF16),
            pltpu.VMEM((g1, 8, LANES), F32),
            pltpu.VMEM((g1, 8, LANES), F32),
            pltpu.VMEM((8, LANES), F32),
            pltpu.VMEM((m_count, 8, LANES), F32),
            dma((8,)), dma((8,)), dma((2,)), dma((2,)), dma((2,)), dma((2,)), dma((2,)), dma((2,)),
            dma((g1,)), dma((g1,)), dma((m_count,)), dma((m_count,)),
        ],
        compiler_params=pltpu.CompilerParams(
            collective_id=0, has_side_effects=True, vmem_limit_bytes=48 * 1024 * 1024
        ),
    )(
        charge_density.reshape(MODES * ROWS, LANES),
        layer_ids.reshape(ROWS, LANES),
        eps_mean,
        eps_fluct,
        galerkin,
        net_ids.reshape(ROWS, 1),
        net_place.reshape(-1, LANES),
    )
    mine = charges[:, :8].reshape(8, 2, 4)
    charges = jnp.transpose(mine, (1, 0, 2)).reshape(MODES, 4)
    return potential.reshape(charge_density.shape), charges


def solution(mesh):
    return jax.shard_map(
        functools.partial(local, mesh.shape["gx"], mesh.shape["gy"]),
        mesh=mesh,
        in_specs=(
            P(None, None, "gx", "gy"),
            P(None, "gx", "gy"),
            P(),
            P(),
            P(),
            P(None, "gx", "gy"),
            P(),
        ),
        out_specs=(P(None, None, "gx", "gy"), P(None, ("gx", "gy"))),
        check_vma=False,
    )
```

```python
import functools

import jax
import jax.numpy as jnp
from jax import lax
from jax.experimental import pallas as pl
from jax.experimental.pallas import tpu as pltpu
from jax.sharding import PartitionSpec as P

charge_scale = 1.0 / 512.0
relax = 0.8

Y_LO, SZ, CORES = 4, 8, 2
SX, Y_HI = 4, 2
MODES, LAYERS = 16, 8
NZ, ROWS, LANES = 32, 64, 128
CHUNK = 8
MESH = pl.DeviceIdType.MESH
F32, BF16, I32 = jnp.float32, jnp.bfloat16, jnp.int32

BESIDE = ((-1, 0), (1, 0), (0, -1), (0, 1), (-1, -1), (-1, 1), (1, -1), (1, 1))
SLOT = {offset: q for q, offset in enumerate(BESIDE)}


def lanes(shape):
    return lax.broadcasted_iota(I32, shape, len(shape) - 1)


def rows(shape):
    return lax.broadcasted_iota(I32, shape, 0)


def packed(ids):
    return jnp.where(ids < LAYERS, jnp.left_shift(1, (ids & 7) * 4), 0)


def counts(word):
    out = []
    for l in range(LAYERS):
        one = (lax.shift_right_logical(word, 4 * l) & 15).astype(F32)
        out.append(jnp.concatenate([one, one], 0))
    return out


def wide(ref, r):
    return jnp.broadcast_to(ref[pl.ds(r, 1), :], (8, LANES))


def bits(ids):
    two = jnp.concatenate([ids, ids], 0)
    return [(two & (1 << b)) != 0 for b in range(3)]


def pick(mask, parts):
    for m in mask:
        parts = [jnp.where(m, parts[i + 1], parts[i]) for i in range(0, len(parts), 2)]
    return parts[0]


def weigh(cnt, parts):
    total = cnt[0] * parts[0]
    for c, part in zip(cnt[1:], parts[1:]):
        total = total + c * part
    return total


def apply_all(b3, tiles):
    high = [t.astype(BF16) for t in tiles]
    low = [(t - h.astype(F32)).astype(BF16) for t, h in zip(tiles, high)]
    high = jnp.concatenate(high, 1)
    rhs = jnp.concatenate([high, high, jnp.concatenate(low, 1)], 0)
    u = jnp.dot(b3, rhs, preferred_element_type=F32)
    return [
        [u[l * MODES : (l + 1) * MODES, i * LANES : (i + 1) * LANES] for l in range(LAYERS)]
        for i in range(len(tiles))
    ]


def kernel(
    gx_size, gy_size,
    rho_hbm, ids_hbm, mean_hbm, fluct_hbm, g_hbm, net_hbm, place_hbm,
    pot_hbm, charge_ref,
    pot_ref, pot_s,
    rho_ref, ids_ref, mean_ref, fluct_ref, g_ref, net_ref, place_ref, in_s,
    rv, v, w, t, rd, hx, hv, hw, hid, ie, ier, es, er,
    b3_ref, d_ref, idh_ref, cw_ref, chw_ref, c4_ref, oht, s1, r1, s2, r2,
    ie_s, ie_r, hid_s, hid_r, hx_s, hx_r, e_s, e_r, r1_s, r1_r, r2_s, r2_r,
):
    gx, gy = lax.axis_index("gx"), lax.axis_index("gy")
    core, z, y_lo = gx % CORES, (gx // CORES) % SZ, gx // (CORES * SZ)
    x, y_hi = gy // Y_HI, gy % Y_HI
    g1, m_count = SZ * SX, Y_LO * CORES * Y_HI
    group = z * SX + x
    member = (y_lo * CORES + core) * Y_HI + y_hi

    def group_peer(s):
        peer = (group + s) % g1
        return ((y_lo * SZ + peer // SX) * CORES + core, (peer % SX) * Y_HI + y_hi), peer

    def member_peer(s):
        peer = (member + s) % m_count
        lo, c, hi = peer // (CORES * Y_HI), (peer // Y_HI) % CORES, peer % Y_HI
        return ((lo * SZ + z) * CORES + c, x * Y_HI + hi)

    def exists(q):
        dx, dy = BESIDE[q]
        ok = None
        for step, at, size in ((dx, gx, gx_size), (dy, gy, gy_size)):
            if step:
                here = at > 0 if step < 0 else at < size - 1
                ok = here if ok is None else jnp.logical_and(ok, here)
        return ok

    def target(q):
        return (gx + BESIDE[q][0], gy + BESIDE[q][1])

    def back(q):
        return SLOT[(-BESIDE[q][0], -BESIDE[q][1])]

    fetch = [
        pltpu.make_async_copy(source, here, in_s.at[i])
        for i, (source, here) in enumerate((
            (rho_hbm, rho_ref), (ids_hbm, ids_ref), (net_hbm, net_ref), (g_hbm, g_ref),
            (fluct_hbm, fluct_ref), (mean_hbm, mean_ref), (place_hbm, place_ref),
        ))
    ]
    for one in fetch:
        one.start()

    barrier = pltpu.get_barrier_semaphore()
    expected = g1 - 1 + m_count - 1
    for q in range(8):
        expected = expected + exists(q).astype(I32)

        @pl.when(exists(q))
        def _(q=q):
            pl.semaphore_signal(barrier, inc=1, device_id=target(q), device_id_type=MESH)

    @pl.loop(1, g1)
    def _(s):
        pl.semaphore_signal(barrier, inc=1, device_id=group_peer(s)[0], device_id_type=MESH)

    @pl.loop(1, m_count)
    def _(s):
        pl.semaphore_signal(barrier, inc=1, device_id=member_peer(s), device_id_type=MESH)

    lane16 = lanes((MODES, LANES))
    lane1 = lanes((1, LANES))
    lane64, row64 = lanes((ROWS, LANES)), rows((ROWS, LANES))
    on_low = lane64 == 2 * row64
    on_high = lane64 == ((2 * row64 + 127) & 127)

    fetch[1].wait()
    fetch[2].wait()
    own_ids = ids_ref[...]
    ids_f = own_ids.astype(F32)

    def edge_of(low, high):
        both = jnp.where(on_low, low, 0.0) + jnp.where(on_high, high, 0.0)
        return jnp.sum(both, axis=0, keepdims=True).astype(I32)

    net_own = jnp.zeros((1, LANES), F32)
    for x_row in range(2):
        net = jnp.broadcast_to(net_ref[x_row], (8, NZ))
        wanted = 4 * rows((NZ, LANES)) + 2 * x_row
        spread = jnp.logical_or(
            lanes((NZ, LANES)) == wanted, lanes((NZ, LANES)) == ((wanted + 127) & 127)
        ).astype(F32).astype(BF16)
        for part, scale in ((lax.shift_right_logical(net, 3), 8.0), (net & 7, 1.0)):
            part = part.astype(F32).astype(BF16)
            net_own = net_own + scale * jnp.dot(part, spread, preferred_element_type=F32)[0:1]
    net_own = net_own.astype(I32)
    own_edge = edge_of(ids_f[:, 0:1], ids_f[:, 127:128])
    ie[0] = own_edge
    ie[1] = edge_of(ids_f[:, 1:2], ids_f[:, 126:127])
    ie[2] = net_own

    def gather_edge(tile, r, acc):
        mine = jnp.logical_or(lane16 == 2 * r, lane16 == ((2 * r + 127) & 127))
        return jnp.where(mine, pltpu.roll(tile, 2 * r, 1), acc)

    def rearrange(c, acc):
        for i in range(CHUNK):
            r = c * CHUNK + i
            tile = rho_ref[pl.ds(r, MODES, stride=ROWS), :]
            rv[c * (CHUNK // 2) + i // 2, i % 2] = tile
            acc = gather_edge(tile, r, acc)
        return acc

    fetch[0].wait()
    es[...] = lax.fori_loop(0, ROWS // CHUNK, rearrange, jnp.zeros((MODES, LANES), F32))

    pl.semaphore_wait(barrier, expected)

    def rv_x(q):
        return rv.at[:, q]

    def ie_part(ref, q):
        return ref.at[2] if q < 2 else ref if q < 4 else ref.at[0]

    def ie_copy(q):
        return pltpu.make_async_remote_copy(
            ie_part(ie, q), ie_part(ier.at[back(q)], q), ie_s.at[q], ie_r.at[back(q)], device_id=target(q), device_id_type=MESH
        )

    def hid_copy(q):
        return pltpu.make_async_remote_copy(
            ids_ref, hid.at[back(q)], hid_s.at[q], hid_r.at[back(q)], device_id=target(q), device_id_type=MESH
        )

    def hx_copy(q):
        return pltpu.make_async_remote_copy(
            rv_x(q),
            hx.at[back(q)], hx_s.at[q], hx_r.at[back(q)], device_id=target(q), device_id_type=MESH,
        )

    def e_copy(q):
        return pltpu.make_async_remote_copy(
            es, er.at[back(q) - 2], e_s.at[q - 2], e_r.at[back(q) - 2], device_id=target(q), device_id_type=MESH
        )

    def copies(q):
        found = [ie_copy(q)]
        if q < 2:
            found += [hid_copy(q), hx_copy(q)]
        elif q < 4:
            found += [e_copy(q)]
        return found

    for q in (4, 5, 6, 7, 2, 3, 0, 1):
        @pl.when(exists(q))
        def _(q=q):
            for one in copies(q):
                one.start()

        @pl.when(jnp.logical_not(exists(q)))
        def _(q=q):
            for k in (0, 1):
                ier[q, k] = jnp.full((1, LANES), LAYERS, I32)
            ier[q, 2] = jnp.full((1, LANES), -1, I32)
            if q < 2:
                hid[q] = jnp.full((ROWS, LANES), LAYERS, I32)
                hx[q] = jnp.zeros((NZ, MODES, LANES), F32)
            elif q < 4:
                er[q - 2] = jnp.zeros((MODES, LANES), F32)

    for one in fetch[3:6]:
        one.wait()
    for l in range(LAYERS):
        total = g_ref[0]
        for i in range(1, MODES):
            total = total + fluct_ref[l, i - 1] * g_ref[i]
        total = mean_ref[l] * total
        eye = rows((MODES, MODES)) == lanes((MODES, MODES))
        d_ref[l] = jnp.broadcast_to(
            jnp.sum(jnp.where(eye, total, 0.0), axis=1, keepdims=True), (MODES, LANES)
        )
        three = jnp.concatenate([total, total, total], 1)
        high = three.astype(BF16)
        low = (three - high.astype(F32)).astype(BF16).astype(F32)
        at = lanes((MODES, 3 * MODES))
        middle = jnp.logical_and(at >= MODES, at < 2 * MODES)
        b3_ref[pl.ds(l * MODES, MODES), :] = jnp.where(middle, low, high.astype(F32)).astype(BF16)

    zero = jnp.zeros((2, MODES, LANES), F32)
    for ref in (v, w):
        ref[0:2] = zero
        ref[ROWS + 2 : ROWS + 4] = zero

    def wait_recv(q, which):
        @pl.when(exists(q))
        def _():
            pltpu.make_async_remote_copy(
                *which(q), device_id=target(q), device_id_type=MESH
            ).wait_recv()

    def wait_ie(q):
        wait_recv(q, lambda q: (ie_part(ie, q), ie_part(ier.at[q], q), ie_s.at[q], ie_r.at[q]))

    for q in range(4):
        wait_ie(q)
    for q in range(2):
        wait_recv(q, lambda q: (ids_ref, hid.at[q], hid_s.at[q], hid_r.at[q]))

    even64 = (row64 & 1) == 0
    left, right = hid[0], hid[1]

    def row_swap(low, high):
        return jnp.where(even64, pltpu.roll(low, ROWS - 1, 0), pltpu.roll(high, 1, 0))

    halo_ids = row_swap(left, right)
    outer_ids = jnp.where(even64, left, right)
    idh_ref[...] = halo_ids

    def roll1(row, by):
        return pltpu.roll(jnp.broadcast_to(row, (8, LANES)), by % LANES, 1)[0:1]

    quarter = lane1 & 3

    def beside_row(k):
        from_left, from_right = ier[2, k], ier[3, k]
        return jnp.where((lane1 & 1) == 0, roll1(from_left, 1), roll1(from_right, -1))

    edge_ids, edge_ids2 = beside_row(0), beside_row(1)

    def to_column(row, mask):
        return jnp.sum(jnp.where(mask, row.astype(F32), 0.0), axis=1, keepdims=True).astype(I32)

    def around_y(p, edge_row):
        word = packed(edge_row)
        low = jnp.bitwise_and(word, 0xFFFF)
        high = lax.shift_right_logical(word, 16)

        def column(mask):
            return to_column(low, mask) + jnp.left_shift(to_column(high, mask), 16)

        below = jnp.where(lane64 == 0, column(on_low), pltpu.roll(p, 1, 1))
        above = jnp.where(lane64 == LANES - 1, column(on_high), pltpu.roll(p, LANES - 1, 1))
        return below + above

    def around_z(p):
        up = jnp.where(row64 < ROWS - 2, pltpu.roll(p, ROWS - 2, 0), 0)
        return up + jnp.where(row64 >= 2, pltpu.roll(p, 2, 0), 0)

    p_own, p_halo = packed(own_ids), packed(halo_ids)
    four = around_z(p_own) + row_swap(p_own, p_own) + p_halo
    c4_ref[...] = four + 4 * p_own
    cw_ref[...] = four + around_y(p_own, edge_ids) + 6 * p_own
    b3 = b3_ref[...]

    def start(rho, word):
        cnt = counts(word)
        inverse = (2.0 * relax) / weigh(cnt, [d_ref[l] for l in range(LAYERS)])
        return rho * inverse, inverse, cnt

    @pl.loop(0, ROWS // CHUNK)
    def _(c):
        tiles, cnts = [], []
        for i in range(CHUNK):
            r = c * CHUNK + i
            tile, inverse, cnt = start(rv[c * (CHUNK // 2) + i // 2, i % 2], wide(cw_ref, r))
            rd[r] = inverse
            v[r + 2] = tile
            tiles.append(tile)
            cnts.append(cnt)
        u = apply_all(b3, tiles)
        for i in range(CHUNK):
            r = c * CHUNK + i
            w[r + 2] = pick(bits(wide(ids_ref, r)), u[i])
            t[r] = weigh(cnts[i], u[i])

    fetch[6].wait()
    odd_from = jnp.where(quarter == 3, roll1(ier[0, 2], -2), roll1(ier[1, 2], 2))
    nets = (
        jnp.where((lane1 & 1) == 0, net_own, odd_from),
        jnp.where((lane1 & 1) == 0, ier[2, 2], ier[3, 2]),
        net_own,
    )
    place = place_ref[...]
    place_parts = jnp.concatenate(
        [lax.shift_right_logical(place, 3).astype(F32), (place & 7).astype(F32)], 0
    ).astype(BF16)
    hi_rows = place.shape[0]
    columns = []
    for net in nets:
        chosen = (rows((LANES, LANES)) == (net & (LANES - 1))).astype(F32).astype(BF16)
        found = jnp.dot(place_parts, chosen, preferred_element_type=F32)
        value = 8.0 * found[:hi_rows] + found[hi_rows:]
        own_row = rows((hi_rows, LANES)) == lax.shift_right_logical(net, 7)
        column = jnp.sum(jnp.where(own_row, value, 0.0), axis=0, keepdims=True)
        columns.append(jnp.where(net < 0, -1.0, column).astype(I32))

    spot = rows((LANES, LANES))
    spot_m, spot_g, spot_c = spot // 8, (spot // 4) & 1, spot & 3
    per_gx = gy_size * 4
    spot_p = (
        ((spot_m // (CORES * Y_HI)) * SZ * CORES + (spot_m // Y_HI) % CORES) * per_gx
        + (spot_g * Y_HI + spot_m % Y_HI) * 4 + spot_c
    )
    spot_p = jnp.where(spot_m < m_count, spot_p, -2)

    @pl.loop(0, g1 // 2)
    def _(pair):
        base = (2 * pair // SX) * CORES * per_gx + ((2 * pair) % SX) * Y_HI * 4
        for b, column in enumerate(columns):
            hit = spot_p == column - base
            hit = jnp.logical_and(hit, spot_p >= 0)
            oht[pl.ds(pl.multiple_of(pair * LANES, LANES), LANES), b * LANES : (b + 1) * LANES] = (
                jnp.where(hit, 1.0, 0.0).astype(BF16)
            )

    for q in range(4, 8):
        wait_ie(q)
    ll, lr, rl, rr = (ier[q, 0] for q in (4, 5, 6, 7))
    edge_halo = jnp.where(
        quarter == 0, roll1(ll, -1),
        jnp.where(quarter == 2, roll1(rl, 3), jnp.where(quarter == 3, roll1(lr, -3), roll1(rr, 1))),
    )
    chw_ref[...] = (
        around_z(p_halo) + p_own + packed(outer_ids) + around_y(p_halo, edge_halo) + 6 * p_halo
    )

    edge_z = lax.shift_right_logical((lane1 + 1) & (LANES - 1), 2)
    p_edge = packed(edge_ids)
    edge_low_x = jnp.logical_or(quarter == 0, quarter == 3)
    edge_word = (
        jnp.where(edge_z > 0, roll1(p_edge, 4), 0)
        + jnp.where(edge_z < NZ - 1, roll1(p_edge, -4), 0)
        + jnp.where(edge_low_x, roll1(p_edge, -2), roll1(p_edge, 2))
        + packed(edge_halo) + packed(own_edge) + packed(edge_ids2) + 6 * p_edge
    )

    for q in range(2):
        wait_recv(q, lambda q: (rv_x(q), hx.at[q], hx_s.at[q], hx_r.at[q]))

    @pl.loop(0, ROWS // CHUNK)
    def _(c):
        tiles = []
        for i in range(CHUNK):
            r = c * CHUNK + i
            tile, _, _ = start(hx[i % 2, c * (CHUNK // 2) + i // 2], wide(chw_ref, r))
            hv[r] = tile
            tiles.append(tile)
        u = apply_all(b3, tiles)
        for i in range(CHUNK):
            r = c * CHUNK + i
            hw[r] = pick(bits(wide(idh_ref, r)), u[i])

    for q in range(2, 4):
        wait_recv(q, lambda q: (es, er.at[q - 2], e_s.at[q - 2], e_r.at[q - 2]))

    even16 = (lane16 & 1) == 0
    edge_rho = jnp.where(even16, pltpu.roll(er[0], 1, 1), pltpu.roll(er[1], LANES - 1, 1))
    edge_v, _, _ = start(edge_rho, jnp.broadcast_to(edge_word, (8, LANES)))
    edge_bits = bits(jnp.broadcast_to(edge_ids, (8, LANES)))
    edge_w = pick(edge_bits, apply_all(b3, [edge_v])[0])

    def beside_y(tile, edge, r):
        mine = pltpu.roll(edge, (LANES - 2 * r) & (LANES - 1), 1)
        below = jnp.where(lane16 == 0, mine, pltpu.roll(tile, 1, 1))
        return below + jnp.where(lane16 == LANES - 1, mine, pltpu.roll(tile, LANES - 1, 1))

    def within(ref, c, i):
        r = c * CHUNK + i
        return ref[r] + ref[r + 4] + ref[c * CHUNK + (i ^ 1) + 2]

    @pl.loop(0, ROWS // CHUNK)
    def _(c):
        tiles = []
        for i in range(CHUNK):
            r = c * CHUNK + i
            tiles.append(within(v, c, i) + hv[r] + beside_y(v[r + 2], edge_v, r))
        u = apply_all(b3, tiles)
        for i in range(CHUNK):
            r = c * CHUNK + i
            near = within(w, c, i) + hw[r] + beside_y(w[r + 2], edge_w, r)
            flux = 0.5 * (t[r] - pick(bits(wide(ids_ref, r)), u[i]) - near)
            result = v[r + 2] + rd[r] * (rv[c * (CHUNK // 2) + i // 2, i % 2] - flux)
            hv[r] = result
            pot_ref[pl.ds(r, MODES, stride=ROWS), :] = result

    put = pltpu.make_async_copy(pot_ref, pot_hbm, pot_s)
    put.start()

    @pl.loop(0, ROWS // CHUNK, init_carry=(jnp.zeros((MODES, LANES), F32),) * 2)
    def sums(c, carry):
        acc, edge = carry
        tiles = [hv[c * CHUNK + i] for i in range(CHUNK)]
        u = apply_all(b3, tiles)
        for i in range(CHUNK):
            r = c * CHUNK + i
            v[r + 2] = tiles[i]
            edge = gather_edge(tiles[i], r, edge)
            own = pick(bits(wide(ids_ref, r)), u[i])
            w[r + 2] = own
            t[r] = weigh(counts(wide(c4_ref, r)), u[i])
            out = own + pick(bits(wide(idh_ref, r)), u[i])
            total = -0.5 * jnp.sum(out, axis=1, keepdims=True)
            acc = jnp.where(lane16 == ((2 * r + 127) & 127), total, acc)
        return acc, edge

    acc, edge_p = sums

    @pl.loop(0, ROWS // CHUNK, init_carry=acc)
    def acc(c, acc):
        u = apply_all(b3, [within(v, c, i) for i in range(CHUNK)])
        for i in range(CHUNK):
            r = c * CHUNK + i
            flux = t[r] - pick(bits(wide(ids_ref, r)), u[i]) - within(w, c, i)
            total = 0.5 * jnp.sum(flux, axis=1, keepdims=True)
            acc = jnp.where(lane16 == 2 * r, total, acc)
        return acc

    u = apply_all(b3, [edge_p])[0]
    inside = jnp.broadcast_to(edge_ids, (MODES, LANES)) < LAYERS
    across = 0.5 * (
        pick(bits(jnp.broadcast_to(own_edge, (8, LANES))), u) + jnp.where(inside, pick(edge_bits, u), 0.0)
    )
    blocks = jnp.concatenate([acc, -across, across], 1) * charge_scale
    high = blocks.astype(BF16)
    low = (blocks - high.astype(F32)).astype(BF16)
    parts = jnp.concatenate([high, low], 0)

    alternate = (lanes((8, LANES)) & 4) == 0

    placed = lax.dot_general(
        parts, oht[...], (((1,), (1,)), ((), ())), preferred_element_type=F32
    )
    placed = placed[:MODES] + placed[MODES:]
    for pair in range(g1 // 2):
        a = placed[0:8, pair * LANES : (pair + 1) * LANES]
        b = placed[8:16, pair * LANES : (pair + 1) * LANES]
        s1[2 * pair] = jnp.where(alternate, a, pltpu.roll(b, 4, 1))
        s1[2 * pair + 1] = jnp.where(alternate, pltpu.roll(a, LANES - 4, 1), b)

    def r1_copy(s):
        device, peer = group_peer(s)
        return pltpu.make_async_remote_copy(
            s1.at[peer], r1.at[s], r1_s.at[s], r1_r.at[s], device_id=device, device_id_type=MESH
        )

    def r2_copy(s):
        return pltpu.make_async_remote_copy(
            s2, r2.at[s], r2_s.at[s], r2_r.at[s], device_id=member_peer(s), device_id_type=MESH
        )

    @pl.loop(1, g1)
    def _(s):
        r1_copy(s).start()

    @pl.loop(1, g1, init_carry=s1[group])
    def share(s, total):
        r1_copy(s).wait_recv()
        return total + r1[s]

    s2[...] = share

    @pl.loop(1, m_count)
    def _(s):
        r2_copy(s).start()

    @pl.loop(1, m_count, init_carry=share)
    def final(s, total):
        r2_copy(s).wait_recv()
        return total + r2[s]

    turned = pltpu.roll(final, (LANES - 8 * member) & (LANES - 1), 1)
    turned = turned.T
    charge_ref[...] = jnp.concatenate([turned[0:4], turned[4:8]], 1)

    @pl.loop(1, g1)
    def _(s):
        r1_copy(s).wait_send()

    @pl.loop(1, m_count)
    def _(s):
        r2_copy(s).wait_send()

    for q in range(8):
        @pl.when(exists(q))
        def _(q=q):
            for one in copies(q):
                one.wait_send()

    put.wait()


def local(gx_size, gy_size, charge_density, layer_ids, eps_mean, eps_fluct, galerkin, net_ids, net_place):
    vmem = pl.BlockSpec(memory_space=pltpu.VMEM)
    hbm = pl.BlockSpec(memory_space=pltpu.HBM)
    g1, m_count = SZ * SX, Y_LO * CORES * Y_HI
    tile = (MODES, LANES)
    dma = pltpu.SemaphoreType.DMA
    potential, charges = pl.pallas_call(
        functools.partial(kernel, gx_size, gy_size),
        out_shape=(
            jax.ShapeDtypeStruct((MODES * ROWS, LANES), F32),
            jax.ShapeDtypeStruct((4, MODES), F32),
        ),
        in_specs=[hbm] * 7,
        out_specs=(hbm, vmem),
        scratch_shapes=[
            pltpu.VMEM((MODES * ROWS, LANES), F32),
            pltpu.SemaphoreType.DMA,
            pltpu.VMEM((MODES * ROWS, LANES), F32),
            pltpu.VMEM((ROWS, LANES), I32),
            pltpu.SMEM((LAYERS,), F32),
            pltpu.SMEM((LAYERS, MODES - 1), F32),
            pltpu.VMEM((MODES,) * 3, F32),
            pltpu.VMEM((2, 1, NZ), I32),
            pltpu.VMEM((net_place.shape[0] // LANES, LANES), I32),
            pltpu.SemaphoreType.DMA((7,)),
            pltpu.VMEM((NZ, 2) + tile, F32),
            pltpu.VMEM((ROWS + 4,) + tile, F32),
            pltpu.VMEM((ROWS + 4,) + tile, F32),
            pltpu.VMEM((ROWS,) + tile, F32),
            pltpu.VMEM((ROWS,) + tile, F32),
            pltpu.VMEM((2, NZ) + tile, F32),
            pltpu.VMEM((ROWS,) + tile, F32),
            pltpu.VMEM((ROWS,) + tile, F32),
            pltpu.VMEM((2, ROWS, LANES), I32),
            pltpu.VMEM((3, 1, LANES), I32),
            pltpu.VMEM((8, 3, 1, LANES), I32),
            pltpu.VMEM(tile, F32),
            pltpu.VMEM((2,) + tile, F32),
            pltpu.VMEM((LAYERS * MODES, 3 * MODES), BF16),
            pltpu.VMEM((LAYERS,) + tile, F32),
            pltpu.VMEM((ROWS, LANES), I32),
            pltpu.VMEM((ROWS, LANES), I32),
            pltpu.VMEM((ROWS, LANES), I32),
            pltpu.VMEM((ROWS, LANES), I32),
            pltpu.VMEM((g1 // 2 * LANES, 3 * LANES), BF16),
            pltpu.VMEM((g1, 8, LANES), F32),
            pltpu.VMEM((g1, 8, LANES), F32),
            pltpu.VMEM((8, LANES), F32),
            pltpu.VMEM((m_count, 8, LANES), F32),
            dma((8,)), dma((8,)), dma((2,)), dma((2,)), dma((2,)), dma((2,)), dma((2,)), dma((2,)),
            dma((g1,)), dma((g1,)), dma((m_count,)), dma((m_count,)),
        ],
        compiler_params=pltpu.CompilerParams(
            collective_id=0, has_side_effects=True, vmem_limit_bytes=67043328
        ),
    )(
        charge_density.reshape(MODES * ROWS, LANES),
        layer_ids.reshape(ROWS, LANES),
        eps_mean,
        eps_fluct,
        galerkin,
        jnp.transpose(net_ids, (1, 2, 0)),
        net_place.reshape(-1, LANES),
    )
    return potential.reshape(charge_density.shape), charges.T


def solution(mesh):
    return jax.shard_map(
        functools.partial(local, mesh.shape["gx"], mesh.shape["gy"]),
        mesh=mesh,
        in_specs=(
            P(None, None, "gx", "gy"),
            P(None, "gx", "gy"),
            P(),
            P(),
            P(),
            P(None, "gx", "gy"),
            P(),
        ),
        out_specs=(P(None, None, "gx", "gy"), P(None, ("gx", "gy"))),
        check_vma=False,
    )
```

```python
import functools

import jax
import jax.numpy as jnp
from jax import lax
from jax.experimental import pallas as pl
from jax.experimental.pallas import tpu as pltpu
from jax.sharding import PartitionSpec as P

charge_scale = 1.0 / 512.0
relax = 0.8

Y_LO, SZ, CORES = 4, 8, 2
SX, Y_HI = 4, 2
MODES, LAYERS = 16, 8
NZ, ROWS, LANES = 32, 64, 128
CHUNK = 32
MESH = pl.DeviceIdType.MESH
F32, BF16, I32 = jnp.float32, jnp.bfloat16, jnp.int32

BESIDE = ((-1, 0), (1, 0), (0, -1), (0, 1), (-1, -1), (-1, 1), (1, -1), (1, 1))
SLOT = {offset: q for q, offset in enumerate(BESIDE)}


def lanes(shape):
    return lax.broadcasted_iota(I32, shape, len(shape) - 1)


def rows(shape):
    return lax.broadcasted_iota(I32, shape, 0)


def packed(ids):
    return jnp.where(ids < LAYERS, jnp.left_shift(1, (ids & 7) * 4), 0)


def counts(word):
    out = []
    for l in range(LAYERS):
        one = (lax.shift_right_logical(word, 4 * l) & 15).astype(F32)
        out.append(jnp.concatenate([one, one], 0))
    return out


def wide(ref, r):
    return jnp.broadcast_to(ref[pl.ds(r, 1), :], (8, LANES))


def bits(ids):
    two = jnp.concatenate([ids, ids], 0)
    return [(two & (1 << b)) != 0 for b in range(3)]


def pick(mask, parts):
    for m in mask:
        parts = [jnp.where(m, parts[i + 1], parts[i]) for i in range(0, len(parts), 2)]
    return parts[0]


def weigh(cnt, parts):
    total = cnt[0] * parts[0]
    for c, part in zip(cnt[1:], parts[1:]):
        total = total + c * part
    return total


def apply_all(b3, tiles):
    high = [t.astype(BF16) for t in tiles]
    low = [(t - h.astype(F32)).astype(BF16) for t, h in zip(tiles, high)]
    high = jnp.concatenate(high, 1)
    rhs = jnp.concatenate([high, high, jnp.concatenate(low, 1)], 0)
    u = jnp.dot(b3, rhs, preferred_element_type=F32)
    return [
        [u[l * MODES : (l + 1) * MODES, i * LANES : (i + 1) * LANES] for l in range(LAYERS)]
        for i in range(len(tiles))
    ]


def kernel(
    gx_size, gy_size,
    rho_hbm, ids_hbm, mean_hbm, fluct_hbm, g_hbm, net_hbm, place_hbm,
    pot_hbm, charge_ref,
    pot_ref, pot_s,
    rho_ref, ids_ref, mean_ref, fluct_ref, g_ref, net_ref, place_ref, in_s,
    rv, v, w, t, rd, hx, hv, hw, hid, ie, ier, es, er,
    b3_ref, d_ref, idh_ref, cw_ref, chw_ref, c4_ref, oht, s1, r1, s2, r2,
    ie_s, ie_r, hid_s, hid_r, hx_s, hx_r, e_s, e_r, r1_s, r1_r, r2_s, r2_r,
):
    gx, gy = lax.axis_index("gx"), lax.axis_index("gy")
    core, z, y_lo = gx % CORES, (gx // CORES) % SZ, gx // (CORES * SZ)
    x, y_hi = gy // Y_HI, gy % Y_HI
    g1, m_count = SZ * SX, Y_LO * CORES * Y_HI
    group = z * SX + x
    member = (y_lo * CORES + core) * Y_HI + y_hi

    def group_peer(s):
        peer = (group + s) % g1
        return ((y_lo * SZ + peer // SX) * CORES + core, (peer % SX) * Y_HI + y_hi), peer

    def member_peer(s):
        peer = (member + s) % m_count
        lo, c, hi = peer // (CORES * Y_HI), (peer // Y_HI) % CORES, peer % Y_HI
        return ((lo * SZ + z) * CORES + c, x * Y_HI + hi)

    def exists(q):
        dx, dy = BESIDE[q]
        ok = None
        for step, at, size in ((dx, gx, gx_size), (dy, gy, gy_size)):
            if step:
                here = at > 0 if step < 0 else at < size - 1
                ok = here if ok is None else jnp.logical_and(ok, here)
        return ok

    def target(q):
        return (gx + BESIDE[q][0], gy + BESIDE[q][1])

    def back(q):
        return SLOT[(-BESIDE[q][0], -BESIDE[q][1])]

    fetch = [
        pltpu.make_async_copy(source, here, in_s.at[i])
        for i, (source, here) in enumerate((
            (rho_hbm, rho_ref), (ids_hbm, ids_ref), (net_hbm, net_ref), (g_hbm, g_ref),
            (fluct_hbm, fluct_ref), (mean_hbm, mean_ref), (place_hbm, place_ref),
        ))
    ]
    for one in fetch:
        one.start()

    barrier = pltpu.get_barrier_semaphore()
    expected = g1 - 1 + m_count - 1
    for q in range(8):
        expected = expected + exists(q).astype(I32)

        @pl.when(exists(q))
        def _(q=q):
            pl.semaphore_signal(barrier, inc=1, device_id=target(q), device_id_type=MESH)

    @pl.loop(1, g1)
    def _(s):
        pl.semaphore_signal(barrier, inc=1, device_id=group_peer(s)[0], device_id_type=MESH)

    @pl.loop(1, m_count)
    def _(s):
        pl.semaphore_signal(barrier, inc=1, device_id=member_peer(s), device_id_type=MESH)

    lane16 = lanes((MODES, LANES))
    lane1 = lanes((1, LANES))
    lane64, row64 = lanes((ROWS, LANES)), rows((ROWS, LANES))
    on_low = lane64 == 2 * row64
    on_high = lane64 == ((2 * row64 + 127) & 127)

    fetch[1].wait()
    fetch[2].wait()
    own_ids = ids_ref[...]
    ids_f = own_ids.astype(F32)

    def edge_of(low, high):
        both = jnp.where(on_low, low, 0.0) + jnp.where(on_high, high, 0.0)
        return jnp.sum(both, axis=0, keepdims=True).astype(I32)

    net_own = jnp.zeros((1, LANES), F32)
    for x_row in range(2):
        net = jnp.broadcast_to(net_ref[x_row], (8, NZ))
        wanted = 4 * rows((NZ, LANES)) + 2 * x_row
        spread = jnp.logical_or(
            lanes((NZ, LANES)) == wanted, lanes((NZ, LANES)) == ((wanted + 127) & 127)
        ).astype(F32).astype(BF16)
        for part, scale in ((lax.shift_right_logical(net, 3), 8.0), (net & 7, 1.0)):
            part = part.astype(F32).astype(BF16)
            net_own = net_own + scale * jnp.dot(part, spread, preferred_element_type=F32)[0:1]
    net_own = net_own.astype(I32)
    own_edge = edge_of(ids_f[:, 0:1], ids_f[:, 127:128])
    ie[0] = own_edge
    ie[1] = edge_of(ids_f[:, 1:2], ids_f[:, 126:127])
    ie[2] = net_own

    def gather_edge(tile, r, acc):
        mine = jnp.logical_or(lane16 == 2 * r, lane16 == ((2 * r + 127) & 127))
        return jnp.where(mine, pltpu.roll(tile, 2 * r, 1), acc)

    def rearrange(c, acc):
        for i in range(CHUNK):
            r = c * CHUNK + i
            tile = rho_ref[pl.ds(r, MODES, stride=ROWS), :]
            rv[c * (CHUNK // 2) + i // 2, i % 2] = tile
            acc = gather_edge(tile, r, acc)
        return acc

    fetch[0].wait()
    es[...] = lax.fori_loop(0, ROWS // CHUNK, rearrange, jnp.zeros((MODES, LANES), F32))

    pl.semaphore_wait(barrier, expected)

    def rv_x(q):
        return rv.at[:, q]

    def ie_part(ref, q):
        return ref.at[2] if q < 2 else ref if q < 4 else ref.at[0]

    def ie_copy(q):
        return pltpu.make_async_remote_copy(
            ie_part(ie, q), ie_part(ier.at[back(q)], q), ie_s.at[q], ie_r.at[back(q)], device_id=target(q), device_id_type=MESH
        )

    def hid_copy(q):
        return pltpu.make_async_remote_copy(
            ids_ref, hid.at[back(q)], hid_s.at[q], hid_r.at[back(q)], device_id=target(q), device_id_type=MESH
        )

    def hx_copy(q):
        return pltpu.make_async_remote_copy(
            rv_x(q),
            hx.at[back(q)], hx_s.at[q], hx_r.at[back(q)], device_id=target(q), device_id_type=MESH,
        )

    def e_copy(q):
        return pltpu.make_async_remote_copy(
            es, er.at[back(q) - 2], e_s.at[q - 2], e_r.at[back(q) - 2], device_id=target(q), device_id_type=MESH
        )

    def copies(q):
        found = [ie_copy(q)]
        if q < 2:
            found += [hid_copy(q), hx_copy(q)]
        elif q < 4:
            found += [e_copy(q)]
        return found

    for q in (4, 5, 6, 7, 2, 3, 0, 1):
        @pl.when(exists(q))
        def _(q=q):
            for one in copies(q):
                one.start()

        @pl.when(jnp.logical_not(exists(q)))
        def _(q=q):
            for k in (0, 1):
                ier[q, k] = jnp.full((1, LANES), LAYERS, I32)
            ier[q, 2] = jnp.full((1, LANES), -1, I32)
            if q < 2:
                hid[q] = jnp.full((ROWS, LANES), LAYERS, I32)
                hx[q] = jnp.zeros((NZ, MODES, LANES), F32)
            elif q < 4:
                er[q - 2] = jnp.zeros((MODES, LANES), F32)

    for one in fetch[3:6]:
        one.wait()
    for l in range(LAYERS):
        total = g_ref[0]
        for i in range(1, MODES):
            total = total + fluct_ref[l, i - 1] * g_ref[i]
        total = mean_ref[l] * total
        eye = rows((MODES, MODES)) == lanes((MODES, MODES))
        d_ref[l] = jnp.broadcast_to(
            jnp.sum(jnp.where(eye, total, 0.0), axis=1, keepdims=True), (MODES, LANES)
        )
        three = jnp.concatenate([total, total, total], 1)
        high = three.astype(BF16)
        low = (three - high.astype(F32)).astype(BF16).astype(F32)
        at = lanes((MODES, 3 * MODES))
        middle = jnp.logical_and(at >= MODES, at < 2 * MODES)
        b3_ref[pl.ds(l * MODES, MODES), :] = jnp.where(middle, low, high.astype(F32)).astype(BF16)

    zero = jnp.zeros((2, MODES, LANES), F32)
    for ref in (v, w):
        ref[0:2] = zero
        ref[ROWS + 2 : ROWS + 4] = zero

    def wait_recv(q, which):
        @pl.when(exists(q))
        def _():
            pltpu.make_async_remote_copy(
                *which(q), device_id=target(q), device_id_type=MESH
            ).wait_recv()

    def wait_ie(q):
        wait_recv(q, lambda q: (ie_part(ie, q), ie_part(ier.at[q], q), ie_s.at[q], ie_r.at[q]))

    for q in range(4):
        wait_ie(q)
    for q in range(2):
        wait_recv(q, lambda q: (ids_ref, hid.at[q], hid_s.at[q], hid_r.at[q]))

    even64 = (row64 & 1) == 0
    left, right = hid[0], hid[1]

    def row_swap(low, high):
        return jnp.where(even64, pltpu.roll(low, ROWS - 1, 0), pltpu.roll(high, 1, 0))

    halo_ids = row_swap(left, right)
    outer_ids = jnp.where(even64, left, right)
    idh_ref[...] = halo_ids

    def roll1(row, by):
        return pltpu.roll(jnp.broadcast_to(row, (8, LANES)), by % LANES, 1)[0:1]

    quarter = lane1 & 3

    def beside_row(k):
        from_left, from_right = ier[2, k], ier[3, k]
        return jnp.where((lane1 & 1) == 0, roll1(from_left, 1), roll1(from_right, -1))

    edge_ids, edge_ids2 = beside_row(0), beside_row(1)

    def to_column(row, mask):
        return jnp.sum(jnp.where(mask, row.astype(F32), 0.0), axis=1, keepdims=True).astype(I32)

    def around_y(p, edge_row):
        word = packed(edge_row)
        low = jnp.bitwise_and(word, 0xFFFF)
        high = lax.shift_right_logical(word, 16)

        def column(mask):
            return to_column(low, mask) + jnp.left_shift(to_column(high, mask), 16)

        below = jnp.where(lane64 == 0, column(on_low), pltpu.roll(p, 1, 1))
        above = jnp.where(lane64 == LANES - 1, column(on_high), pltpu.roll(p, LANES - 1, 1))
        return below + above

    def around_z(p):
        up = jnp.where(row64 < ROWS - 2, pltpu.roll(p, ROWS - 2, 0), 0)
        return up + jnp.where(row64 >= 2, pltpu.roll(p, 2, 0), 0)

    p_own, p_halo = packed(own_ids), packed(halo_ids)
    four = around_z(p_own) + row_swap(p_own, p_own) + p_halo
    c4_ref[...] = four + 4 * p_own
    cw_ref[...] = four + around_y(p_own, edge_ids) + 6 * p_own
    b3 = b3_ref[...]

    def start(rho, word):
        cnt = counts(word)
        inverse = (2.0 * relax) / weigh(cnt, [d_ref[l] for l in range(LAYERS)])
        return rho * inverse, inverse, cnt

    @pl.loop(0, ROWS // CHUNK)
    def _(c):
        tiles, cnts = [], []
        for i in range(CHUNK):
            r = c * CHUNK + i
            tile, inverse, cnt = start(rv[c * (CHUNK // 2) + i // 2, i % 2], wide(cw_ref, r))
            rd[r] = inverse
            v[r + 2] = tile
            tiles.append(tile)
            cnts.append(cnt)
        u = apply_all(b3, tiles)
        for i in range(CHUNK):
            r = c * CHUNK + i
            w[r + 2] = pick(bits(wide(ids_ref, r)), u[i])
            t[r] = weigh(cnts[i], u[i])

    fetch[6].wait()
    odd_from = jnp.where(quarter == 3, roll1(ier[0, 2], -2), roll1(ier[1, 2], 2))
    nets = (
        jnp.where((lane1 & 1) == 0, net_own, odd_from),
        jnp.where((lane1 & 1) == 0, ier[2, 2], ier[3, 2]),
        net_own,
    )
    place = place_ref[...]
    place_parts = jnp.concatenate(
        [lax.shift_right_logical(place, 3).astype(F32), (place & 7).astype(F32)], 0
    ).astype(BF16)
    hi_rows = place.shape[0]
    columns = []
    for net in nets:
        chosen = (rows((LANES, LANES)) == (net & (LANES - 1))).astype(F32).astype(BF16)
        found = jnp.dot(place_parts, chosen, preferred_element_type=F32)
        value = 8.0 * found[:hi_rows] + found[hi_rows:]
        own_row = rows((hi_rows, LANES)) == lax.shift_right_logical(net, 7)
        column = jnp.sum(jnp.where(own_row, value, 0.0), axis=0, keepdims=True)
        columns.append(jnp.where(net < 0, -1.0, column).astype(I32))

    spot = rows((LANES, LANES))
    spot_m, spot_g, spot_c = spot // 8, (spot // 4) & 1, spot & 3
    per_gx = gy_size * 4
    spot_p = (
        ((spot_m // (CORES * Y_HI)) * SZ * CORES + (spot_m // Y_HI) % CORES) * per_gx
        + (spot_g * Y_HI + spot_m % Y_HI) * 4 + spot_c
    )
    spot_p = jnp.where(spot_m < m_count, spot_p, -2)

    @pl.loop(0, g1 // 2)
    def _(pair):
        base = (2 * pair // SX) * CORES * per_gx + ((2 * pair) % SX) * Y_HI * 4
        for b, column in enumerate(columns):
            hit = spot_p == column - base
            hit = jnp.logical_and(hit, spot_p >= 0)
            oht[pl.ds(pl.multiple_of(pair * LANES, LANES), LANES), b * LANES : (b + 1) * LANES] = (
                jnp.where(hit, 1.0, 0.0).astype(BF16)
            )

    for q in range(4, 8):
        wait_ie(q)
    ll, lr, rl, rr = (ier[q, 0] for q in (4, 5, 6, 7))
    edge_halo = jnp.where(
        quarter == 0, roll1(ll, -1),
        jnp.where(quarter == 2, roll1(rl, 3), jnp.where(quarter == 3, roll1(lr, -3), roll1(rr, 1))),
    )
    chw_ref[...] = (
        around_z(p_halo) + p_own + packed(outer_ids) + around_y(p_halo, edge_halo) + 6 * p_halo
    )

    edge_z = lax.shift_right_logical((lane1 + 1) & (LANES - 1), 2)
    p_edge = packed(edge_ids)
    edge_low_x = jnp.logical_or(quarter == 0, quarter == 3)
    edge_word = (
        jnp.where(edge_z > 0, roll1(p_edge, 4), 0)
        + jnp.where(edge_z < NZ - 1, roll1(p_edge, -4), 0)
        + jnp.where(edge_low_x, roll1(p_edge, -2), roll1(p_edge, 2))
        + packed(edge_halo) + packed(own_edge) + packed(edge_ids2) + 6 * p_edge
    )

    for q in range(2):
        wait_recv(q, lambda q: (rv_x(q), hx.at[q], hx_s.at[q], hx_r.at[q]))

    @pl.loop(0, ROWS // CHUNK)
    def _(c):
        tiles = []
        for i in range(CHUNK):
            r = c * CHUNK + i
            tile, _, _ = start(hx[i % 2, c * (CHUNK // 2) + i // 2], wide(chw_ref, r))
            hv[r] = tile
            tiles.append(tile)
        u = apply_all(b3, tiles)
        for i in range(CHUNK):
            r = c * CHUNK + i
            hw[r] = pick(bits(wide(idh_ref, r)), u[i])

    for q in range(2, 4):
        wait_recv(q, lambda q: (es, er.at[q - 2], e_s.at[q - 2], e_r.at[q - 2]))

    even16 = (lane16 & 1) == 0
    edge_rho = jnp.where(even16, pltpu.roll(er[0], 1, 1), pltpu.roll(er[1], LANES - 1, 1))
    edge_v, _, _ = start(edge_rho, jnp.broadcast_to(edge_word, (8, LANES)))
    edge_bits = bits(jnp.broadcast_to(edge_ids, (8, LANES)))
    edge_w = pick(edge_bits, apply_all(b3, [edge_v])[0])

    def beside_y(tile, edge, r):
        mine = pltpu.roll(edge, (LANES - 2 * r) & (LANES - 1), 1)
        below = jnp.where(lane16 == 0, mine, pltpu.roll(tile, 1, 1))
        return below + jnp.where(lane16 == LANES - 1, mine, pltpu.roll(tile, LANES - 1, 1))

    def within(ref, c, i):
        r = c * CHUNK + i
        return ref[r] + ref[r + 4] + ref[c * CHUNK + (i ^ 1) + 2]

    @pl.loop(0, ROWS // CHUNK)
    def _(c):
        tiles = []
        for i in range(CHUNK):
            r = c * CHUNK + i
            tiles.append(within(v, c, i) + hv[r] + beside_y(v[r + 2], edge_v, r))
        u = apply_all(b3, tiles)
        for i in range(CHUNK):
            r = c * CHUNK + i
            near = within(w, c, i) + hw[r] + beside_y(w[r + 2], edge_w, r)
            flux = 0.5 * (t[r] - pick(bits(wide(ids_ref, r)), u[i]) - near)
            result = v[r + 2] + rd[r] * (rv[c * (CHUNK // 2) + i // 2, i % 2] - flux)
            hv[r] = result
            pot_ref[pl.ds(r, MODES, stride=ROWS), :] = result

    put = pltpu.make_async_copy(pot_ref, pot_hbm, pot_s)
    put.start()

    @pl.loop(0, ROWS // CHUNK, init_carry=(jnp.zeros((MODES, LANES), F32),) * 2)
    def sums(c, carry):
        acc, edge = carry
        tiles = [hv[c * CHUNK + i] for i in range(CHUNK)]
        u = apply_all(b3, tiles)
        for i in range(CHUNK):
            r = c * CHUNK + i
            v[r + 2] = tiles[i]
            edge = gather_edge(tiles[i], r, edge)
            own = pick(bits(wide(ids_ref, r)), u[i])
            w[r + 2] = own
            t[r] = weigh(counts(wide(c4_ref, r)), u[i])
            out = own + pick(bits(wide(idh_ref, r)), u[i])
            total = -0.5 * jnp.sum(out, axis=1, keepdims=True)
            acc = jnp.where(lane16 == ((2 * r + 127) & 127), total, acc)
        return acc, edge

    acc, edge_p = sums

    @pl.loop(0, ROWS // CHUNK, init_carry=acc)
    def acc(c, acc):
        u = apply_all(b3, [within(v, c, i) for i in range(CHUNK)])
        for i in range(CHUNK):
            r = c * CHUNK + i
            flux = t[r] - pick(bits(wide(ids_ref, r)), u[i]) - within(w, c, i)
            total = 0.5 * jnp.sum(flux, axis=1, keepdims=True)
            acc = jnp.where(lane16 == 2 * r, total, acc)
        return acc

    u = apply_all(b3, [edge_p])[0]
    inside = jnp.broadcast_to(edge_ids, (MODES, LANES)) < LAYERS
    across = 0.5 * (
        pick(bits(jnp.broadcast_to(own_edge, (8, LANES))), u) + jnp.where(inside, pick(edge_bits, u), 0.0)
    )
    blocks = jnp.concatenate([acc, -across, across], 1) * charge_scale
    high = blocks.astype(BF16)
    low = (blocks - high.astype(F32)).astype(BF16)
    parts = jnp.concatenate([high, low], 0)

    alternate = (lanes((8, LANES)) & 4) == 0

    placed = lax.dot_general(
        parts, oht[...], (((1,), (1,)), ((), ())), preferred_element_type=F32
    )
    placed = placed[:MODES] + placed[MODES:]
    for pair in range(g1 // 2):
        a = placed[0:8, pair * LANES : (pair + 1) * LANES]
        b = placed[8:16, pair * LANES : (pair + 1) * LANES]
        s1[2 * pair] = jnp.where(alternate, a, pltpu.roll(b, 4, 1))
        s1[2 * pair + 1] = jnp.where(alternate, pltpu.roll(a, LANES - 4, 1), b)

    def r1_copy(s):
        device, peer = group_peer(s)
        return pltpu.make_async_remote_copy(
            s1.at[peer], r1.at[s], r1_s.at[s], r1_r.at[s], device_id=device, device_id_type=MESH
        )

    def r2_copy(s):
        return pltpu.make_async_remote_copy(
            s2, r2.at[s], r2_s.at[s], r2_r.at[s], device_id=member_peer(s), device_id_type=MESH
        )

    @pl.loop(1, g1)
    def _(s):
        r1_copy(s).start()

    @pl.loop(1, g1, init_carry=s1[group])
    def share(s, total):
        r1_copy(s).wait_recv()
        return total + r1[s]

    s2[...] = share

    @pl.loop(1, m_count)
    def _(s):
        r2_copy(s).start()

    @pl.loop(1, m_count, init_carry=share)
    def final(s, total):
        r2_copy(s).wait_recv()
        return total + r2[s]

    turned = pltpu.roll(final, (LANES - 8 * member) & (LANES - 1), 1)
    turned = turned.T
    charge_ref[...] = jnp.concatenate([turned[0:4], turned[4:8]], 1)

    @pl.loop(1, g1)
    def _(s):
        r1_copy(s).wait_send()

    @pl.loop(1, m_count)
    def _(s):
        r2_copy(s).wait_send()

    for q in range(8):
        @pl.when(exists(q))
        def _(q=q):
            for one in copies(q):
                one.wait_send()

    put.wait()


def local(gx_size, gy_size, charge_density, layer_ids, eps_mean, eps_fluct, galerkin, net_ids, net_place):
    vmem = pl.BlockSpec(memory_space=pltpu.VMEM)
    hbm = pl.BlockSpec(memory_space=pltpu.HBM)
    g1, m_count = SZ * SX, Y_LO * CORES * Y_HI
    tile = (MODES, LANES)
    dma = pltpu.SemaphoreType.DMA
    potential, charges = pl.pallas_call(
        functools.partial(kernel, gx_size, gy_size),
        out_shape=(
            jax.ShapeDtypeStruct((MODES * ROWS, LANES), F32),
            jax.ShapeDtypeStruct((4, MODES), F32),
        ),
        in_specs=[hbm] * 7,
        out_specs=(hbm, vmem),
        scratch_shapes=[
            pltpu.VMEM((MODES * ROWS, LANES), F32),
            pltpu.SemaphoreType.DMA,
            pltpu.VMEM((MODES * ROWS, LANES), F32),
            pltpu.VMEM((ROWS, LANES), I32),
            pltpu.SMEM((LAYERS,), F32),
            pltpu.SMEM((LAYERS, MODES - 1), F32),
            pltpu.VMEM((MODES,) * 3, F32),
            pltpu.VMEM((2, 1, NZ), I32),
            pltpu.VMEM((net_place.shape[0] // LANES, LANES), I32),
            pltpu.SemaphoreType.DMA((7,)),
            pltpu.VMEM((NZ, 2) + tile, F32),
            pltpu.VMEM((ROWS + 4,) + tile, F32),
            pltpu.VMEM((ROWS + 4,) + tile, F32),
            pltpu.VMEM((ROWS,) + tile, F32),
            pltpu.VMEM((ROWS,) + tile, F32),
            pltpu.VMEM((2, NZ) + tile, F32),
            pltpu.VMEM((ROWS,) + tile, F32),
            pltpu.VMEM((ROWS,) + tile, F32),
            pltpu.VMEM((2, ROWS, LANES), I32),
            pltpu.VMEM((3, 1, LANES), I32),
            pltpu.VMEM((8, 3, 1, LANES), I32),
            pltpu.VMEM(tile, F32),
            pltpu.VMEM((2,) + tile, F32),
            pltpu.VMEM((LAYERS * MODES, 3 * MODES), BF16),
            pltpu.VMEM((LAYERS,) + tile, F32),
            pltpu.VMEM((ROWS, LANES), I32),
            pltpu.VMEM((ROWS, LANES), I32),
            pltpu.VMEM((ROWS, LANES), I32),
            pltpu.VMEM((ROWS, LANES), I32),
            pltpu.VMEM((g1 // 2 * LANES, 3 * LANES), BF16),
            pltpu.VMEM((g1, 8, LANES), F32),
            pltpu.VMEM((g1, 8, LANES), F32),
            pltpu.VMEM((8, LANES), F32),
            pltpu.VMEM((m_count, 8, LANES), F32),
            dma((8,)), dma((8,)), dma((2,)), dma((2,)), dma((2,)), dma((2,)), dma((2,)), dma((2,)),
            dma((g1,)), dma((g1,)), dma((m_count,)), dma((m_count,)),
        ],
        compiler_params=pltpu.CompilerParams(
            collective_id=0, has_side_effects=True, vmem_limit_bytes=67043328
        ),
    )(
        charge_density.reshape(MODES * ROWS, LANES),
        layer_ids.reshape(ROWS, LANES),
        eps_mean,
        eps_fluct,
        galerkin,
        jnp.transpose(net_ids, (1, 2, 0)),
        net_place.reshape(-1, LANES),
    )
    return potential.reshape(charge_density.shape), charges.T


def solution(mesh):
    return jax.shard_map(
        functools.partial(local, mesh.shape["gx"], mesh.shape["gy"]),
        mesh=mesh,
        in_specs=(
            P(None, None, "gx", "gy"),
            P(None, "gx", "gy"),
            P(),
            P(),
            P(),
            P(None, "gx", "gy"),
            P(),
        ),
        out_specs=(P(None, None, "gx", "gy"), P(None, ("gx", "gy"))),
        check_vma=False,
    )
```

```python
import functools

import jax
import jax.numpy as jnp
from jax import lax
from jax.experimental import pallas as pl
from jax.experimental.pallas import tpu as pltpu
from jax.sharding import PartitionSpec as P

charge_scale = 1.0 / 512.0
relax = 0.8

Y_LO, SZ, CORES = 4, 8, 2
SX, Y_HI = 4, 2
MODES, LAYERS = 16, 8
NZ, ROWS, LANES = 32, 64, 128
CHUNK = 64
MESH = pl.DeviceIdType.MESH
F32, BF16, I32 = jnp.float32, jnp.bfloat16, jnp.int32

BESIDE = ((-1, 0), (1, 0), (0, -1), (0, 1), (-1, -1), (-1, 1), (1, -1), (1, 1))
SLOT = {offset: q for q, offset in enumerate(BESIDE)}


def lanes(shape):
    return lax.broadcasted_iota(I32, shape, len(shape) - 1)


def rows(shape):
    return lax.broadcasted_iota(I32, shape, 0)


def packed(ids):
    return jnp.where(ids < LAYERS, jnp.left_shift(1, (ids & 7) * 4), 0)


def counts(word):
    out = []
    for l in range(LAYERS):
        one = (lax.shift_right_logical(word, 4 * l) & 15).astype(F32)
        out.append(jnp.concatenate([one, one], 0))
    return out


def wide(ref, r):
    return jnp.broadcast_to(ref[pl.ds(r, 1), :], (8, LANES))


def bits(ids):
    two = jnp.concatenate([ids, ids], 0)
    return [(two & (1 << b)) != 0 for b in range(3)]


def pick(mask, parts):
    for m in mask:
        parts = [jnp.where(m, parts[i + 1], parts[i]) for i in range(0, len(parts), 2)]
    return parts[0]


def weigh(cnt, parts):
    total = cnt[0] * parts[0]
    for c, part in zip(cnt[1:], parts[1:]):
        total = total + c * part
    return total


def apply_all(b3, tiles):
    high = [t.astype(BF16) for t in tiles]
    low = [(t - h.astype(F32)).astype(BF16) for t, h in zip(tiles, high)]
    high = jnp.concatenate(high, 1)
    rhs = jnp.concatenate([high, high, jnp.concatenate(low, 1)], 0)
    u = jnp.dot(b3, rhs, preferred_element_type=F32)
    return [
        [u[l * MODES : (l + 1) * MODES, i * LANES : (i + 1) * LANES] for l in range(LAYERS)]
        for i in range(len(tiles))
    ]


def kernel(
    gx_size, gy_size,
    rho_hbm, ids_hbm, mean_hbm, fluct_hbm, g_hbm, net_hbm, place_hbm,
    pot_hbm, charge_ref,
    pot_ref, pot_s,
    rho_ref, ids_ref, mean_ref, fluct_ref, g_ref, net_ref, place_ref, in_s,
    rv, v, w, t, rd, hx, hv, hw, hid, ie, ier, es, er,
    b3_ref, d_ref, idh_ref, cw_ref, chw_ref, c4_ref, oht, s1, r1, s2, r2,
    ie_s, ie_r, hid_s, hid_r, hx_s, hx_r, e_s, e_r, r1_s, r1_r, r2_s, r2_r,
):
    gx, gy = lax.axis_index("gx"), lax.axis_index("gy")
    core, z, y_lo = gx % CORES, (gx // CORES) % SZ, gx // (CORES * SZ)
    x, y_hi = gy // Y_HI, gy % Y_HI
    g1, m_count = SZ * SX, Y_LO * CORES * Y_HI
    group = z * SX + x
    member = (y_lo * CORES + core) * Y_HI + y_hi

    def group_peer(s):
        peer = (group + s) % g1
        return ((y_lo * SZ + peer // SX) * CORES + core, (peer % SX) * Y_HI + y_hi), peer

    def member_peer(s):
        peer = (member + s) % m_count
        lo, c, hi = peer // (CORES * Y_HI), (peer // Y_HI) % CORES, peer % Y_HI
        return ((lo * SZ + z) * CORES + c, x * Y_HI + hi)

    def exists(q):
        dx, dy = BESIDE[q]
        ok = None
        for step, at, size in ((dx, gx, gx_size), (dy, gy, gy_size)):
            if step:
                here = at > 0 if step < 0 else at < size - 1
                ok = here if ok is None else jnp.logical_and(ok, here)
        return ok

    def target(q):
        return (gx + BESIDE[q][0], gy + BESIDE[q][1])

    def back(q):
        return SLOT[(-BESIDE[q][0], -BESIDE[q][1])]

    fetch = [
        pltpu.make_async_copy(source, here, in_s.at[i])
        for i, (source, here) in enumerate((
            (rho_hbm, rho_ref), (ids_hbm, ids_ref), (net_hbm, net_ref), (g_hbm, g_ref),
            (fluct_hbm, fluct_ref), (mean_hbm, mean_ref), (place_hbm, place_ref),
        ))
    ]
    for one in fetch:
        one.start()

    barrier = pltpu.get_barrier_semaphore()
    expected = g1 - 1 + m_count - 1
    for q in range(8):
        expected = expected + exists(q).astype(I32)

        @pl.when(exists(q))
        def _(q=q):
            pl.semaphore_signal(barrier, inc=1, device_id=target(q), device_id_type=MESH)

    for s in range(1, g1):
        pl.semaphore_signal(barrier, inc=1, device_id=group_peer(s)[0], device_id_type=MESH)

    for s in range(1, m_count):
        pl.semaphore_signal(barrier, inc=1, device_id=member_peer(s), device_id_type=MESH)

    lane16 = lanes((MODES, LANES))
    lane1 = lanes((1, LANES))
    lane64, row64 = lanes((ROWS, LANES)), rows((ROWS, LANES))
    on_low = lane64 == 2 * row64
    on_high = lane64 == ((2 * row64 + 127) & 127)

    fetch[1].wait()
    fetch[2].wait()
    own_ids = ids_ref[...]
    ids_f = own_ids.astype(F32)

    def edge_of(low, high):
        both = jnp.where(on_low, low, 0.0) + jnp.where(on_high, high, 0.0)
        return jnp.sum(both, axis=0, keepdims=True).astype(I32)

    net_own = jnp.zeros((1, LANES), F32)
    for x_row in range(2):
        net = jnp.broadcast_to(net_ref[x_row], (8, NZ))
        wanted = 4 * rows((NZ, LANES)) + 2 * x_row
        spread = jnp.logical_or(
            lanes((NZ, LANES)) == wanted, lanes((NZ, LANES)) == ((wanted + 127) & 127)
        ).astype(F32).astype(BF16)
        for part, scale in ((lax.shift_right_logical(net, 3), 8.0), (net & 7, 1.0)):
            part = part.astype(F32).astype(BF16)
            net_own = net_own + scale * jnp.dot(part, spread, preferred_element_type=F32)[0:1]
    net_own = net_own.astype(I32)
    own_edge = edge_of(ids_f[:, 0:1], ids_f[:, 127:128])
    ie[0] = own_edge
    ie[1] = edge_of(ids_f[:, 1:2], ids_f[:, 126:127])
    ie[2] = net_own

    def gather_edge(tile, r, acc):
        mine = jnp.logical_or(lane16 == 2 * r, lane16 == ((2 * r + 127) & 127))
        return jnp.where(mine, pltpu.roll(tile, 2 * r, 1), acc)

    def rearrange(c, acc):
        for i in range(CHUNK):
            r = c * CHUNK + i
            tile = rho_ref[pl.ds(r, MODES, stride=ROWS), :]
            rv[c * (CHUNK // 2) + i // 2, i % 2] = tile
            acc = gather_edge(tile, r, acc)
        return acc

    fetch[0].wait()
    es[...] = lax.fori_loop(0, ROWS // CHUNK, rearrange, jnp.zeros((MODES, LANES), F32))

    pl.semaphore_wait(barrier, expected)

    def rv_x(q):
        return rv.at[:, q]

    def ie_part(ref, q):
        return ref.at[2] if q < 2 else ref if q < 4 else ref.at[0]

    def ie_copy(q):
        return pltpu.make_async_remote_copy(
            ie_part(ie, q), ie_part(ier.at[back(q)], q), ie_s.at[q], ie_r.at[back(q)], device_id=target(q), device_id_type=MESH
        )

    def hid_copy(q):
        return pltpu.make_async_remote_copy(
            ids_ref, hid.at[back(q)], hid_s.at[q], hid_r.at[back(q)], device_id=target(q), device_id_type=MESH
        )

    def hx_copy(q):
        return pltpu.make_async_remote_copy(
            rv_x(q),
            hx.at[back(q)], hx_s.at[q], hx_r.at[back(q)], device_id=target(q), device_id_type=MESH,
        )

    def e_copy(q):
        return pltpu.make_async_remote_copy(
            es, er.at[back(q) - 2], e_s.at[q - 2], e_r.at[back(q) - 2], device_id=target(q), device_id_type=MESH
        )

    def copies(q):
        found = [ie_copy(q)]
        if q < 2:
            found += [hid_copy(q), hx_copy(q)]
        elif q < 4:
            found += [e_copy(q)]
        return found

    for q in (4, 5, 6, 7, 2, 3, 0, 1):
        @pl.when(exists(q))
        def _(q=q):
            for one in copies(q):
                one.start()

        @pl.when(jnp.logical_not(exists(q)))
        def _(q=q):
            for k in (0, 1):
                ier[q, k] = jnp.full((1, LANES), LAYERS, I32)
            ier[q, 2] = jnp.full((1, LANES), -1, I32)
            if q < 2:
                hid[q] = jnp.full((ROWS, LANES), LAYERS, I32)
                hx[q] = jnp.zeros((NZ, MODES, LANES), F32)
            elif q < 4:
                er[q - 2] = jnp.zeros((MODES, LANES), F32)

    for one in fetch[3:6]:
        one.wait()
    for l in range(LAYERS):
        total = g_ref[0]
        for i in range(1, MODES):
            total = total + fluct_ref[l, i - 1] * g_ref[i]
        total = mean_ref[l] * total
        eye = rows((MODES, MODES)) == lanes((MODES, MODES))
        d_ref[l] = jnp.broadcast_to(
            jnp.sum(jnp.where(eye, total, 0.0), axis=1, keepdims=True), (MODES, LANES)
        )
        three = jnp.concatenate([total, total, total], 1)
        high = three.astype(BF16)
        low = (three - high.astype(F32)).astype(BF16).astype(F32)
        at = lanes((MODES, 3 * MODES))
        middle = jnp.logical_and(at >= MODES, at < 2 * MODES)
        b3_ref[pl.ds(l * MODES, MODES), :] = jnp.where(middle, low, high.astype(F32)).astype(BF16)

    zero = jnp.zeros((2, MODES, LANES), F32)
    for ref in (v, w):
        ref[0:2] = zero
        ref[ROWS + 2 : ROWS + 4] = zero

    def wait_recv(q, which):
        @pl.when(exists(q))
        def _():
            pltpu.make_async_remote_copy(
                *which(q), device_id=target(q), device_id_type=MESH
            ).wait_recv()

    def wait_ie(q):
        wait_recv(q, lambda q: (ie_part(ie, q), ie_part(ier.at[q], q), ie_s.at[q], ie_r.at[q]))

    for q in range(4):
        wait_ie(q)
    for q in range(2):
        wait_recv(q, lambda q: (ids_ref, hid.at[q], hid_s.at[q], hid_r.at[q]))

    even64 = (row64 & 1) == 0
    left, right = hid[0], hid[1]

    def row_swap(low, high):
        return jnp.where(even64, pltpu.roll(low, ROWS - 1, 0), pltpu.roll(high, 1, 0))

    halo_ids = row_swap(left, right)
    outer_ids = jnp.where(even64, left, right)
    idh_ref[...] = halo_ids

    def roll1(row, by):
        return pltpu.roll(jnp.broadcast_to(row, (8, LANES)), by % LANES, 1)[0:1]

    quarter = lane1 & 3

    def beside_row(k):
        from_left, from_right = ier[2, k], ier[3, k]
        return jnp.where((lane1 & 1) == 0, roll1(from_left, 1), roll1(from_right, -1))

    edge_ids, edge_ids2 = beside_row(0), beside_row(1)

    def to_column(row, mask):
        return jnp.sum(jnp.where(mask, row.astype(F32), 0.0), axis=1, keepdims=True).astype(I32)

    def around_y(p, edge_row):
        word = packed(edge_row)
        low = jnp.bitwise_and(word, 0xFFFF)
        high = lax.shift_right_logical(word, 16)

        def column(mask):
            return to_column(low, mask) + jnp.left_shift(to_column(high, mask), 16)

        below = jnp.where(lane64 == 0, column(on_low), pltpu.roll(p, 1, 1))
        above = jnp.where(lane64 == LANES - 1, column(on_high), pltpu.roll(p, LANES - 1, 1))
        return below + above

    def around_z(p):
        up = jnp.where(row64 < ROWS - 2, pltpu.roll(p, ROWS - 2, 0), 0)
        return up + jnp.where(row64 >= 2, pltpu.roll(p, 2, 0), 0)

    p_own, p_halo = packed(own_ids), packed(halo_ids)
    four = around_z(p_own) + row_swap(p_own, p_own) + p_halo
    c4_ref[...] = four + 4 * p_own
    cw_ref[...] = four + around_y(p_own, edge_ids) + 6 * p_own
    b3 = b3_ref[...]

    def start(rho, word):
        cnt = counts(word)
        inverse = (2.0 * relax) / weigh(cnt, [d_ref[l] for l in range(LAYERS)])
        return rho * inverse, inverse, cnt

    @pl.loop(0, ROWS // CHUNK)
    def _(c):
        tiles, cnts = [], []
        for i in range(CHUNK):
            r = c * CHUNK + i
            tile, inverse, cnt = start(rv[c * (CHUNK // 2) + i // 2, i % 2], wide(cw_ref, r))
            rd[r] = inverse
            v[r + 2] = tile
            tiles.append(tile)
            cnts.append(cnt)
        u = apply_all(b3, tiles)
        for i in range(CHUNK):
            r = c * CHUNK + i
            w[r + 2] = pick(bits(wide(ids_ref, r)), u[i])
            t[r] = weigh(cnts[i], u[i])

    fetch[6].wait()
    odd_from = jnp.where(quarter == 3, roll1(ier[0, 2], -2), roll1(ier[1, 2], 2))
    nets = (
        jnp.where((lane1 & 1) == 0, net_own, odd_from),
        jnp.where((lane1 & 1) == 0, ier[2, 2], ier[3, 2]),
        net_own,
    )
    place = place_ref[...]
    place_parts = jnp.concatenate(
        [lax.shift_right_logical(place, 3).astype(F32), (place & 7).astype(F32)], 0
    ).astype(BF16)
    hi_rows = place.shape[0]
    columns = []
    for net in nets:
        chosen = (rows((LANES, LANES)) == (net & (LANES - 1))).astype(F32).astype(BF16)
        found = jnp.dot(place_parts, chosen, preferred_element_type=F32)
        value = 8.0 * found[:hi_rows] + found[hi_rows:]
        own_row = rows((hi_rows, LANES)) == lax.shift_right_logical(net, 7)
        column = jnp.sum(jnp.where(own_row, value, 0.0), axis=0, keepdims=True)
        columns.append(jnp.where(net < 0, -1.0, column).astype(I32))

    spot = rows((LANES, LANES))
    spot_m, spot_g, spot_c = spot // 8, (spot // 4) & 1, spot & 3
    per_gx = gy_size * 4
    spot_p = (
        ((spot_m // (CORES * Y_HI)) * SZ * CORES + (spot_m // Y_HI) % CORES) * per_gx
        + (spot_g * Y_HI + spot_m % Y_HI) * 4 + spot_c
    )
    spot_p = jnp.where(spot_m < m_count, spot_p, -2)

    @pl.loop(0, g1 // 2)
    def _(pair):
        base = (2 * pair // SX) * CORES * per_gx + ((2 * pair) % SX) * Y_HI * 4
        for b, column in enumerate(columns):
            hit = spot_p == column - base
            hit = jnp.logical_and(hit, spot_p >= 0)
            oht[pl.ds(pl.multiple_of(pair * LANES, LANES), LANES), b * LANES : (b + 1) * LANES] = (
                jnp.where(hit, 1.0, 0.0).astype(BF16)
            )

    for q in range(4, 8):
        wait_ie(q)
    ll, lr, rl, rr = (ier[q, 0] for q in (4, 5, 6, 7))
    edge_halo = jnp.where(
        quarter == 0, roll1(ll, -1),
        jnp.where(quarter == 2, roll1(rl, 3), jnp.where(quarter == 3, roll1(lr, -3), roll1(rr, 1))),
    )
    chw_ref[...] = (
        around_z(p_halo) + p_own + packed(outer_ids) + around_y(p_halo, edge_halo) + 6 * p_halo
    )

    edge_z = lax.shift_right_logical((lane1 + 1) & (LANES - 1), 2)
    p_edge = packed(edge_ids)
    edge_low_x = jnp.logical_or(quarter == 0, quarter == 3)
    edge_word = (
        jnp.where(edge_z > 0, roll1(p_edge, 4), 0)
        + jnp.where(edge_z < NZ - 1, roll1(p_edge, -4), 0)
        + jnp.where(edge_low_x, roll1(p_edge, -2), roll1(p_edge, 2))
        + packed(edge_halo) + packed(own_edge) + packed(edge_ids2) + 6 * p_edge
    )

    for q in range(2):
        wait_recv(q, lambda q: (rv_x(q), hx.at[q], hx_s.at[q], hx_r.at[q]))

    @pl.loop(0, ROWS // CHUNK)
    def _(c):
        tiles = []
        for i in range(CHUNK):
            r = c * CHUNK + i
            tile, _, _ = start(hx[i % 2, c * (CHUNK // 2) + i // 2], wide(chw_ref, r))
            hv[r] = tile
            tiles.append(tile)
        u = apply_all(b3, tiles)
        for i in range(CHUNK):
            r = c * CHUNK + i
            hw[r] = pick(bits(wide(idh_ref, r)), u[i])

    for q in range(2, 4):
        wait_recv(q, lambda q: (es, er.at[q - 2], e_s.at[q - 2], e_r.at[q - 2]))

    even16 = (lane16 & 1) == 0
    edge_rho = jnp.where(even16, pltpu.roll(er[0], 1, 1), pltpu.roll(er[1], LANES - 1, 1))
    edge_v, _, _ = start(edge_rho, jnp.broadcast_to(edge_word, (8, LANES)))
    edge_bits = bits(jnp.broadcast_to(edge_ids, (8, LANES)))
    edge_w = pick(edge_bits, apply_all(b3, [edge_v])[0])

    def beside_y(tile, edge, r):
        mine = pltpu.roll(edge, (LANES - 2 * r) & (LANES - 1), 1)
        below = jnp.where(lane16 == 0, mine, pltpu.roll(tile, 1, 1))
        return below + jnp.where(lane16 == LANES - 1, mine, pltpu.roll(tile, LANES - 1, 1))

    def within(ref, c, i):
        r = c * CHUNK + i
        return ref[r] + ref[r + 4] + ref[c * CHUNK + (i ^ 1) + 2]

    @pl.loop(0, ROWS // CHUNK)
    def _(c):
        tiles = []
        for i in range(CHUNK):
            r = c * CHUNK + i
            tiles.append(within(v, c, i) + hv[r] + beside_y(v[r + 2], edge_v, r))
        u = apply_all(b3, tiles)
        for i in range(CHUNK):
            r = c * CHUNK + i
            near = within(w, c, i) + hw[r] + beside_y(w[r + 2], edge_w, r)
            flux = 0.5 * (t[r] - pick(bits(wide(ids_ref, r)), u[i]) - near)
            result = v[r + 2] + rd[r] * (rv[c * (CHUNK // 2) + i // 2, i % 2] - flux)
            hv[r] = result
            pot_ref[pl.ds(r, MODES, stride=ROWS), :] = result

    put = pltpu.make_async_copy(pot_ref, pot_hbm, pot_s)
    put.start()

    @pl.loop(0, ROWS // CHUNK, init_carry=(jnp.zeros((MODES, LANES), F32),) * 2)
    def sums(c, carry):
        acc, edge = carry
        tiles = [hv[c * CHUNK + i] for i in range(CHUNK)]
        u = apply_all(b3, tiles)
        for i in range(CHUNK):
            r = c * CHUNK + i
            v[r + 2] = tiles[i]
            edge = gather_edge(tiles[i], r, edge)
            own = pick(bits(wide(ids_ref, r)), u[i])
            w[r + 2] = own
            t[r] = weigh(counts(wide(c4_ref, r)), u[i])
            out = own + pick(bits(wide(idh_ref, r)), u[i])
            total = -0.5 * jnp.sum(out, axis=1, keepdims=True)
            acc = jnp.where(lane16 == ((2 * r + 127) & 127), total, acc)
        return acc, edge

    acc, edge_p = sums

    @pl.loop(0, ROWS // CHUNK, init_carry=acc)
    def acc(c, acc):
        u = apply_all(b3, [within(v, c, i) for i in range(CHUNK)])
        for i in range(CHUNK):
            r = c * CHUNK + i
            flux = t[r] - pick(bits(wide(ids_ref, r)), u[i]) - within(w, c, i)
            total = 0.5 * jnp.sum(flux, axis=1, keepdims=True)
            acc = jnp.where(lane16 == 2 * r, total, acc)
        return acc

    u = apply_all(b3, [edge_p])[0]
    inside = jnp.broadcast_to(edge_ids, (MODES, LANES)) < LAYERS
    across = 0.5 * (
        pick(bits(jnp.broadcast_to(own_edge, (8, LANES))), u) + jnp.where(inside, pick(edge_bits, u), 0.0)
    )
    blocks = jnp.concatenate([acc, -across, across], 1) * charge_scale
    high = blocks.astype(BF16)
    low = (blocks - high.astype(F32)).astype(BF16)
    parts = jnp.concatenate([high, low], 0)

    alternate = (lanes((8, LANES)) & 4) == 0

    placed = lax.dot_general(
        parts, oht[...], (((1,), (1,)), ((), ())), preferred_element_type=F32
    )
    placed = placed[:MODES] + placed[MODES:]
    for pair in range(g1 // 2):
        a = placed[0:8, pair * LANES : (pair + 1) * LANES]
        b = placed[8:16, pair * LANES : (pair + 1) * LANES]
        s1[2 * pair] = jnp.where(alternate, a, pltpu.roll(b, 4, 1))
        s1[2 * pair + 1] = jnp.where(alternate, pltpu.roll(a, LANES - 4, 1), b)

    def r1_copy(s):
        device, peer = group_peer(s)
        return pltpu.make_async_remote_copy(
            s1.at[peer], r1.at[s], r1_s.at[s], r1_r.at[s], device_id=device, device_id_type=MESH
        )

    def r2_copy(s):
        return pltpu.make_async_remote_copy(
            s2, r2.at[s], r2_s.at[s], r2_r.at[s], device_id=member_peer(s), device_id_type=MESH
        )

    for s in range(1, g1):
        r1_copy(s).start()

    @pl.loop(1, g1, init_carry=s1[group])
    def share(s, total):
        r1_copy(s).wait_recv()
        return total + r1[s]

    s2[...] = share

    for s in range(1, m_count):
        r2_copy(s).start()

    @pl.loop(1, m_count, init_carry=share)
    def final(s, total):
        r2_copy(s).wait_recv()
        return total + r2[s]

    turned = pltpu.roll(final, (LANES - 8 * member) & (LANES - 1), 1)
    turned = turned.T
    charge_ref[...] = jnp.concatenate([turned[0:4], turned[4:8]], 1)

    @pl.loop(1, g1)
    def _(s):
        r1_copy(s).wait_send()

    @pl.loop(1, m_count)
    def _(s):
        r2_copy(s).wait_send()

    for q in range(8):
        @pl.when(exists(q))
        def _(q=q):
            for one in copies(q):
                one.wait_send()

    put.wait()


def local(gx_size, gy_size, charge_density, layer_ids, eps_mean, eps_fluct, galerkin, net_ids, net_place):
    vmem = pl.BlockSpec(memory_space=pltpu.VMEM)
    hbm = pl.BlockSpec(memory_space=pltpu.HBM)
    g1, m_count = SZ * SX, Y_LO * CORES * Y_HI
    tile = (MODES, LANES)
    dma = pltpu.SemaphoreType.DMA
    potential, charges = pl.pallas_call(
        functools.partial(kernel, gx_size, gy_size),
        out_shape=(
            jax.ShapeDtypeStruct((MODES * ROWS, LANES), F32),
            jax.ShapeDtypeStruct((4, MODES), F32),
        ),
        in_specs=[hbm] * 7,
        out_specs=(hbm, vmem),
        scratch_shapes=[
            pltpu.VMEM((MODES * ROWS, LANES), F32),
            pltpu.SemaphoreType.DMA,
            pltpu.VMEM((MODES * ROWS, LANES), F32),
            pltpu.VMEM((ROWS, LANES), I32),
            pltpu.SMEM((LAYERS,), F32),
            pltpu.SMEM((LAYERS, MODES - 1), F32),
            pltpu.VMEM((MODES,) * 3, F32),
            pltpu.VMEM((2, 1, NZ), I32),
            pltpu.VMEM((net_place.shape[0] // LANES, LANES), I32),
            pltpu.SemaphoreType.DMA((7,)),
            pltpu.VMEM((NZ, 2) + tile, F32),
            pltpu.VMEM((ROWS + 4,) + tile, F32),
            pltpu.VMEM((ROWS + 4,) + tile, F32),
            pltpu.VMEM((ROWS,) + tile, F32),
            pltpu.VMEM((ROWS,) + tile, F32),
            pltpu.VMEM((2, NZ) + tile, F32),
            pltpu.VMEM((ROWS,) + tile, F32),
            pltpu.VMEM((ROWS,) + tile, F32),
            pltpu.VMEM((2, ROWS, LANES), I32),
            pltpu.VMEM((3, 1, LANES), I32),
            pltpu.VMEM((8, 3, 1, LANES), I32),
            pltpu.VMEM(tile, F32),
            pltpu.VMEM((2,) + tile, F32),
            pltpu.VMEM((LAYERS * MODES, 3 * MODES), BF16),
            pltpu.VMEM((LAYERS,) + tile, F32),
            pltpu.VMEM((ROWS, LANES), I32),
            pltpu.VMEM((ROWS, LANES), I32),
            pltpu.VMEM((ROWS, LANES), I32),
            pltpu.VMEM((ROWS, LANES), I32),
            pltpu.VMEM((g1 // 2 * LANES, 3 * LANES), BF16),
            pltpu.VMEM((g1, 8, LANES), F32),
            pltpu.VMEM((g1, 8, LANES), F32),
            pltpu.VMEM((8, LANES), F32),
            pltpu.VMEM((m_count, 8, LANES), F32),
            dma((8,)), dma((8,)), dma((2,)), dma((2,)), dma((2,)), dma((2,)), dma((2,)), dma((2,)),
            dma((g1,)), dma((g1,)), dma((m_count,)), dma((m_count,)),
        ],
        compiler_params=pltpu.CompilerParams(
            collective_id=0, has_side_effects=True, vmem_limit_bytes=67043328
        ),
    )(
        charge_density.reshape(MODES * ROWS, LANES),
        layer_ids.reshape(ROWS, LANES),
        eps_mean,
        eps_fluct,
        galerkin,
        jnp.transpose(net_ids, (1, 2, 0)),
        net_place.reshape(-1, LANES),
    )
    return potential.reshape(charge_density.shape), charges.T


def solution(mesh):
    return jax.shard_map(
        functools.partial(local, mesh.shape["gx"], mesh.shape["gy"]),
        mesh=mesh,
        in_specs=(
            P(None, None, "gx", "gy"),
            P(None, "gx", "gy"),
            P(),
            P(),
            P(),
            P(None, "gx", "gy"),
            P(),
        ),
        out_specs=(P(None, None, "gx", "gy"), P(None, ("gx", "gy"))),
        check_vma=False,
    )
```

```python
import functools

import jax
import jax.numpy as jnp
from jax import lax
from jax.experimental import pallas as pl
from jax.experimental.pallas import tpu as pltpu
from jax.sharding import PartitionSpec as P

charge_scale = 1.0 / 512.0
relax = 0.8

Y_LO, SZ, CORES = 4, 8, 2
SX, Y_HI = 4, 2
MODES, LAYERS = 16, 8
NZ, ROWS, LANES = 32, 64, 128
CHUNK = 64
MESH = pl.DeviceIdType.MESH
F32, BF16, I32 = jnp.float32, jnp.bfloat16, jnp.int32

BESIDE = ((-1, 0), (1, 0), (0, -1), (0, 1), (-1, -1), (-1, 1), (1, -1), (1, 1))
SLOT = {offset: q for q, offset in enumerate(BESIDE)}


def lanes(shape):
    return lax.broadcasted_iota(I32, shape, len(shape) - 1)


def rows(shape):
    return lax.broadcasted_iota(I32, shape, 0)


def packed(ids):
    return jnp.where(ids < LAYERS, jnp.left_shift(1, (ids & 7) * 4), 0)


def counts(word):
    out = []
    for l in range(LAYERS):
        one = (lax.shift_right_logical(word, 4 * l) & 15).astype(F32)
        out.append(jnp.concatenate([one, one], 0))
    return out


def wide(ref, r):
    return jnp.broadcast_to(ref[pl.ds(r, 1), :], (8, LANES))


def bits(ids):
    two = jnp.concatenate([ids, ids], 0)
    return [(two & (1 << b)) != 0 for b in range(3)]


def pick(mask, parts):
    for m in mask:
        parts = [jnp.where(m, parts[i + 1], parts[i]) for i in range(0, len(parts), 2)]
    return parts[0]


def weigh(cnt, parts):
    total = cnt[0] * parts[0]
    for c, part in zip(cnt[1:], parts[1:]):
        total = total + c * part
    return total


def apply_all(b3, tiles):
    high = [t.astype(BF16) for t in tiles]
    low = [(t - h.astype(F32)).astype(BF16) for t, h in zip(tiles, high)]
    high = jnp.concatenate(high, 1)
    rhs = jnp.concatenate([high, high, jnp.concatenate(low, 1)], 0)
    u = jnp.dot(b3, rhs, preferred_element_type=F32)
    return [
        [u[l * MODES : (l + 1) * MODES, i * LANES : (i + 1) * LANES] for l in range(LAYERS)]
        for i in range(len(tiles))
    ]


def kernel(
    gx_size, gy_size,
    rho_hbm, ids_hbm, mean_hbm, fluct_hbm, g_hbm, net_hbm, place_hbm,
    pot_hbm, charge_ref,
    pot_ref, pot_s,
    rho_ref, ids_ref, mean_ref, fluct_ref, g_ref, net_ref, place_ref, in_s,
    rv, v, w, t, rd, hx, hv, hw, hid, ie, ier, es, er,
    b3_ref, d_ref, idh_ref, cw_ref, chw_ref, c4_ref, oht, s1, r1, s2, r2,
    ie_s, ie_r, hid_s, hid_r, hx_s, hx_r, e_s, e_r, r1_s, r1_r, r2_s, r2_r,
):
    gx, gy = lax.axis_index("gx"), lax.axis_index("gy")
    core, z, y_lo = gx % CORES, (gx // CORES) % SZ, gx // (CORES * SZ)
    x, y_hi = gy // Y_HI, gy % Y_HI
    g1, m_count = SZ * SX, Y_LO * CORES * Y_HI
    group = z * SX + x
    member = (y_lo * CORES + core) * Y_HI + y_hi

    def group_peer(s):
        peer = (group + s) % g1
        return ((y_lo * SZ + peer // SX) * CORES + core, (peer % SX) * Y_HI + y_hi), peer

    def member_peer(s):
        peer = (member + s) % m_count
        lo, c, hi = peer // (CORES * Y_HI), (peer // Y_HI) % CORES, peer % Y_HI
        return ((lo * SZ + z) * CORES + c, x * Y_HI + hi)

    def exists(q):
        dx, dy = BESIDE[q]
        ok = None
        for step, at, size in ((dx, gx, gx_size), (dy, gy, gy_size)):
            if step:
                here = at > 0 if step < 0 else at < size - 1
                ok = here if ok is None else jnp.logical_and(ok, here)
        return ok

    def target(q):
        return (gx + BESIDE[q][0], gy + BESIDE[q][1])

    def back(q):
        return SLOT[(-BESIDE[q][0], -BESIDE[q][1])]

    fetch = [
        pltpu.make_async_copy(source, here, in_s.at[i])
        for i, (source, here) in enumerate((
            (rho_hbm, rho_ref), (ids_hbm, ids_ref), (net_hbm, net_ref), (g_hbm, g_ref),
            (fluct_hbm, fluct_ref), (mean_hbm, mean_ref), (place_hbm, place_ref),
        ))
    ]
    for one in fetch:
        one.start()

    barrier = pltpu.get_barrier_semaphore()
    expected = g1 - 1 + m_count - 1
    for q in range(8):
        expected = expected + exists(q).astype(I32)

        @pl.when(exists(q))
        def _(q=q):
            pl.semaphore_signal(barrier, inc=1, device_id=target(q), device_id_type=MESH)

    for s in range(1, g1):
        pl.semaphore_signal(barrier, inc=1, device_id=group_peer(s)[0], device_id_type=MESH)

    for s in range(1, m_count):
        pl.semaphore_signal(barrier, inc=1, device_id=member_peer(s), device_id_type=MESH)

    lane16 = lanes((MODES, LANES))
    lane1 = lanes((1, LANES))
    lane64, row64 = lanes((ROWS, LANES)), rows((ROWS, LANES))
    on_low = lane64 == 2 * row64
    on_high = lane64 == ((2 * row64 + 127) & 127)

    fetch[1].wait()
    fetch[2].wait()
    own_ids = ids_ref[...]
    ids_f = own_ids.astype(F32)

    def edge_of(low, high):
        both = jnp.where(on_low, low, 0.0) + jnp.where(on_high, high, 0.0)
        return jnp.sum(both, axis=0, keepdims=True).astype(I32)

    net_own = jnp.zeros((1, LANES), F32)
    for x_row in range(2):
        net = jnp.broadcast_to(net_ref[x_row], (8, NZ))
        wanted = 4 * rows((NZ, LANES)) + 2 * x_row
        spread = jnp.logical_or(
            lanes((NZ, LANES)) == wanted, lanes((NZ, LANES)) == ((wanted + 127) & 127)
        ).astype(F32).astype(BF16)
        for part, scale in ((lax.shift_right_logical(net, 3), 8.0), (net & 7, 1.0)):
            part = part.astype(F32).astype(BF16)
            net_own = net_own + scale * jnp.dot(part, spread, preferred_element_type=F32)[0:1]
    net_own = net_own.astype(I32)
    own_edge = edge_of(ids_f[:, 0:1], ids_f[:, 127:128])
    ie[0] = own_edge
    ie[1] = edge_of(ids_f[:, 1:2], ids_f[:, 126:127])
    ie[2] = net_own

    def gather_edge(tile, r, acc):
        mine = jnp.logical_or(lane16 == 2 * r, lane16 == ((2 * r + 127) & 127))
        return jnp.where(mine, pltpu.roll(tile, 2 * r, 1), acc)

    def rearrange(c, acc):
        for i in range(CHUNK):
            r = c * CHUNK + i
            tile = rho_ref[pl.ds(r, MODES, stride=ROWS), :]
            rv[c * (CHUNK // 2) + i // 2, i % 2] = tile
            acc = gather_edge(tile, r, acc)
        return acc

    fetch[0].wait()
    es[...] = lax.fori_loop(0, ROWS // CHUNK, rearrange, jnp.zeros((MODES, LANES), F32))

    pl.semaphore_wait(barrier, expected)

    def rv_x(q):
        return rv.at[:, q]

    def ie_part(ref, q):
        return ref.at[2] if q < 2 else ref if q < 4 else ref.at[0]

    def ie_copy(q):
        return pltpu.make_async_remote_copy(
            ie_part(ie, q), ie_part(ier.at[back(q)], q), ie_s.at[q], ie_r.at[back(q)], device_id=target(q), device_id_type=MESH
        )

    def hid_copy(q):
        return pltpu.make_async_remote_copy(
            ids_ref, hid.at[back(q)], hid_s.at[q], hid_r.at[back(q)], device_id=target(q), device_id_type=MESH
        )

    def hx_copy(q):
        return pltpu.make_async_remote_copy(
            rv_x(q),
            hx.at[back(q)], hx_s.at[q], hx_r.at[back(q)], device_id=target(q), device_id_type=MESH,
        )

    def e_copy(q):
        return pltpu.make_async_remote_copy(
            es, er.at[back(q) - 2], e_s.at[q - 2], e_r.at[back(q) - 2], device_id=target(q), device_id_type=MESH
        )

    def copies(q):
        found = [ie_copy(q)]
        if q < 2:
            found += [hid_copy(q), hx_copy(q)]
        elif q < 4:
            found += [e_copy(q)]
        return found

    for q in (2, 3, 0, 1, 4, 5, 6, 7):
        @pl.when(exists(q))
        def _(q=q):
            for one in copies(q):
                one.start()

        @pl.when(jnp.logical_not(exists(q)))
        def _(q=q):
            for k in (0, 1):
                ier[q, k] = jnp.full((1, LANES), LAYERS, I32)
            ier[q, 2] = jnp.full((1, LANES), -1, I32)
            if q < 2:
                hid[q] = jnp.full((ROWS, LANES), LAYERS, I32)
                hx[q] = jnp.zeros((NZ, MODES, LANES), F32)
            elif q < 4:
                er[q - 2] = jnp.zeros((MODES, LANES), F32)

    for one in fetch[3:6]:
        one.wait()
    for l in range(LAYERS):
        total = g_ref[0]
        for i in range(1, MODES):
            total = total + fluct_ref[l, i - 1] * g_ref[i]
        total = mean_ref[l] * total
        eye = rows((MODES, MODES)) == lanes((MODES, MODES))
        d_ref[l] = jnp.broadcast_to(
            jnp.sum(jnp.where(eye, total, 0.0), axis=1, keepdims=True), (MODES, LANES)
        )
        three = jnp.concatenate([total, total, total], 1)
        high = three.astype(BF16)
        low = (three - high.astype(F32)).astype(BF16).astype(F32)
        at = lanes((MODES, 3 * MODES))
        middle = jnp.logical_and(at >= MODES, at < 2 * MODES)
        b3_ref[pl.ds(l * MODES, MODES), :] = jnp.where(middle, low, high.astype(F32)).astype(BF16)

    zero = jnp.zeros((2, MODES, LANES), F32)
    for ref in (v, w):
        ref[0:2] = zero
        ref[ROWS + 2 : ROWS + 4] = zero

    def wait_recv(q, which):
        @pl.when(exists(q))
        def _():
            pltpu.make_async_remote_copy(
                *which(q), device_id=target(q), device_id_type=MESH
            ).wait_recv()

    def wait_ie(q):
        wait_recv(q, lambda q: (ie_part(ie, q), ie_part(ier.at[q], q), ie_s.at[q], ie_r.at[q]))

    for q in range(4):
        wait_ie(q)
    for q in range(2):
        wait_recv(q, lambda q: (ids_ref, hid.at[q], hid_s.at[q], hid_r.at[q]))

    even64 = (row64 & 1) == 0
    left, right = hid[0], hid[1]

    def row_swap(low, high):
        return jnp.where(even64, pltpu.roll(low, ROWS - 1, 0), pltpu.roll(high, 1, 0))

    halo_ids = row_swap(left, right)
    outer_ids = jnp.where(even64, left, right)
    idh_ref[...] = halo_ids

    def roll1(row, by):
        return pltpu.roll(jnp.broadcast_to(row, (8, LANES)), by % LANES, 1)[0:1]

    quarter = lane1 & 3

    def beside_row(k):
        from_left, from_right = ier[2, k], ier[3, k]
        return jnp.where((lane1 & 1) == 0, roll1(from_left, 1), roll1(from_right, -1))

    edge_ids, edge_ids2 = beside_row(0), beside_row(1)

    def to_column(row, mask):
        return jnp.sum(jnp.where(mask, row.astype(F32), 0.0), axis=1, keepdims=True).astype(I32)

    def around_y(p, edge_row):
        word = packed(edge_row)
        low = jnp.bitwise_and(word, 0xFFFF)
        high = lax.shift_right_logical(word, 16)

        def column(mask):
            return to_column(low, mask) + jnp.left_shift(to_column(high, mask), 16)

        below = jnp.where(lane64 == 0, column(on_low), pltpu.roll(p, 1, 1))
        above = jnp.where(lane64 == LANES - 1, column(on_high), pltpu.roll(p, LANES - 1, 1))
        return below + above

    def around_z(p):
        up = jnp.where(row64 < ROWS - 2, pltpu.roll(p, ROWS - 2, 0), 0)
        return up + jnp.where(row64 >= 2, pltpu.roll(p, 2, 0), 0)

    p_own, p_halo = packed(own_ids), packed(halo_ids)
    four = around_z(p_own) + row_swap(p_own, p_own) + p_halo
    c4_ref[...] = four + 4 * p_own
    cw_ref[...] = four + around_y(p_own, edge_ids) + 6 * p_own
    b3 = b3_ref[...]

    def start(rho, word):
        cnt = counts(word)
        inverse = (2.0 * relax) / weigh(cnt, [d_ref[l] for l in range(LAYERS)])
        return rho * inverse, inverse, cnt

    @pl.loop(0, ROWS // CHUNK)
    def _(c):
        tiles, cnts = [], []
        for i in range(CHUNK):
            r = c * CHUNK + i
            tile, inverse, cnt = start(rv[c * (CHUNK // 2) + i // 2, i % 2], wide(cw_ref, r))
            rd[r] = inverse
            v[r + 2] = tile
            tiles.append(tile)
            cnts.append(cnt)
        u = apply_all(b3, tiles)
        for i in range(CHUNK):
            r = c * CHUNK + i
            w[r + 2] = pick(bits(wide(ids_ref, r)), u[i])
            t[r] = weigh(cnts[i], u[i])

    fetch[6].wait()
    odd_from = jnp.where(quarter == 3, roll1(ier[0, 2], -2), roll1(ier[1, 2], 2))
    nets = (
        jnp.where((lane1 & 1) == 0, net_own, odd_from),
        jnp.where((lane1 & 1) == 0, ier[2, 2], ier[3, 2]),
        net_own,
    )
    place = place_ref[...]
    place_parts = jnp.concatenate(
        [lax.shift_right_logical(place, 3).astype(F32), (place & 7).astype(F32)], 0
    ).astype(BF16)
    hi_rows = place.shape[0]
    columns = []
    for net in nets:
        chosen = (rows((LANES, LANES)) == (net & (LANES - 1))).astype(F32).astype(BF16)
        found = jnp.dot(place_parts, chosen, preferred_element_type=F32)
        value = 8.0 * found[:hi_rows] + found[hi_rows:]
        own_row = rows((hi_rows, LANES)) == lax.shift_right_logical(net, 7)
        column = jnp.sum(jnp.where(own_row, value, 0.0), axis=0, keepdims=True)
        columns.append(jnp.where(net < 0, -1.0, column).astype(I32))

    spot = rows((LANES, LANES))
    spot_m, spot_g, spot_c = spot // 8, (spot // 4) & 1, spot & 3
    per_gx = gy_size * 4
    spot_p = (
        ((spot_m // (CORES * Y_HI)) * SZ * CORES + (spot_m // Y_HI) % CORES) * per_gx
        + (spot_g * Y_HI + spot_m % Y_HI) * 4 + spot_c
    )
    spot_p = jnp.where(spot_m < m_count, spot_p, -2)

    for pair in range(g1 // 2):
        base = (2 * pair // SX) * CORES * per_gx + ((2 * pair) % SX) * Y_HI * 4
        for b, column in enumerate(columns):
            hit = spot_p == column - base
            hit = jnp.logical_and(hit, spot_p >= 0)
            oht[pair * LANES : (pair + 1) * LANES, b * LANES : (b + 1) * LANES] = (
                jnp.where(hit, 1.0, 0.0).astype(BF16)
            )

    for q in range(4, 8):
        wait_ie(q)
    ll, lr, rl, rr = (ier[q, 0] for q in (4, 5, 6, 7))
    edge_halo = jnp.where(
        quarter == 0, roll1(ll, -1),
        jnp.where(quarter == 2, roll1(rl, 3), jnp.where(quarter == 3, roll1(lr, -3), roll1(rr, 1))),
    )
    chw_ref[...] = (
        around_z(p_halo) + p_own + packed(outer_ids) + around_y(p_halo, edge_halo) + 6 * p_halo
    )

    edge_z = lax.shift_right_logical((lane1 + 1) & (LANES - 1), 2)
    p_edge = packed(edge_ids)
    edge_low_x = jnp.logical_or(quarter == 0, quarter == 3)
    edge_word = (
        jnp.where(edge_z > 0, roll1(p_edge, 4), 0)
        + jnp.where(edge_z < NZ - 1, roll1(p_edge, -4), 0)
        + jnp.where(edge_low_x, roll1(p_edge, -2), roll1(p_edge, 2))
        + packed(edge_halo) + packed(own_edge) + packed(edge_ids2) + 6 * p_edge
    )

    for q in range(2):
        wait_recv(q, lambda q: (rv_x(q), hx.at[q], hx_s.at[q], hx_r.at[q]))

    @pl.loop(0, ROWS // CHUNK)
    def _(c):
        tiles = []
        for i in range(CHUNK):
            r = c * CHUNK + i
            tile, _, _ = start(hx[i % 2, c * (CHUNK // 2) + i // 2], wide(chw_ref, r))
            hv[r] = tile
            tiles.append(tile)
        u = apply_all(b3, tiles)
        for i in range(CHUNK):
            r = c * CHUNK + i
            hw[r] = pick(bits(wide(idh_ref, r)), u[i])

    for q in range(2, 4):
        wait_recv(q, lambda q: (es, er.at[q - 2], e_s.at[q - 2], e_r.at[q - 2]))

    even16 = (lane16 & 1) == 0
    edge_rho = jnp.where(even16, pltpu.roll(er[0], 1, 1), pltpu.roll(er[1], LANES - 1, 1))
    edge_v, _, _ = start(edge_rho, jnp.broadcast_to(edge_word, (8, LANES)))
    edge_bits = bits(jnp.broadcast_to(edge_ids, (8, LANES)))
    edge_w = pick(edge_bits, apply_all(b3, [edge_v])[0])

    def beside_y(tile, edge, r):
        mine = pltpu.roll(edge, (LANES - 2 * r) & (LANES - 1), 1)
        below = jnp.where(lane16 == 0, mine, pltpu.roll(tile, 1, 1))
        return below + jnp.where(lane16 == LANES - 1, mine, pltpu.roll(tile, LANES - 1, 1))

    def within(ref, c, i):
        r = c * CHUNK + i
        return ref[r] + ref[r + 4] + ref[c * CHUNK + (i ^ 1) + 2]

    @pl.loop(0, ROWS // CHUNK)
    def _(c):
        tiles = []
        for i in range(CHUNK):
            r = c * CHUNK + i
            tiles.append(within(v, c, i) + hv[r] + beside_y(v[r + 2], edge_v, r))
        u = apply_all(b3, tiles)
        for i in range(CHUNK):
            r = c * CHUNK + i
            near = within(w, c, i) + hw[r] + beside_y(w[r + 2], edge_w, r)
            flux = 0.5 * (t[r] - pick(bits(wide(ids_ref, r)), u[i]) - near)
            result = v[r + 2] + rd[r] * (rv[c * (CHUNK // 2) + i // 2, i % 2] - flux)
            hv[r] = result
            pot_ref[pl.ds(r, MODES, stride=ROWS), :] = result

    put = pltpu.make_async_copy(pot_ref, pot_hbm, pot_s)
    put.start()

    @pl.loop(0, ROWS // CHUNK, init_carry=(jnp.zeros((MODES, LANES), F32),) * 2)
    def sums(c, carry):
        acc, edge = carry
        tiles = [hv[c * CHUNK + i] for i in range(CHUNK)]
        u = apply_all(b3, tiles)
        for i in range(CHUNK):
            r = c * CHUNK + i
            v[r + 2] = tiles[i]
            edge = gather_edge(tiles[i], r, edge)
            own = pick(bits(wide(ids_ref, r)), u[i])
            w[r + 2] = own
            t[r] = weigh(counts(wide(c4_ref, r)), u[i])
            out = own + pick(bits(wide(idh_ref, r)), u[i])
            total = -0.5 * jnp.sum(out, axis=1, keepdims=True)
            acc = jnp.where(lane16 == ((2 * r + 127) & 127), total, acc)
        return acc, edge

    acc, edge_p = sums

    @pl.loop(0, ROWS // CHUNK, init_carry=acc)
    def acc(c, acc):
        u = apply_all(b3, [within(v, c, i) for i in range(CHUNK)])
        for i in range(CHUNK):
            r = c * CHUNK + i
            flux = t[r] - pick(bits(wide(ids_ref, r)), u[i]) - within(w, c, i)
            total = 0.5 * jnp.sum(flux, axis=1, keepdims=True)
            acc = jnp.where(lane16 == 2 * r, total, acc)
        return acc

    u = apply_all(b3, [edge_p])[0]
    inside = jnp.broadcast_to(edge_ids, (MODES, LANES)) < LAYERS
    across = 0.5 * (
        pick(bits(jnp.broadcast_to(own_edge, (8, LANES))), u) + jnp.where(inside, pick(edge_bits, u), 0.0)
    )
    blocks = jnp.concatenate([acc, -across, across], 1) * charge_scale
    high = blocks.astype(BF16)
    low = (blocks - high.astype(F32)).astype(BF16)
    parts = jnp.concatenate([high, low], 0)

    alternate = (lanes((8, LANES)) & 4) == 0

    placed = lax.dot_general(
        parts, oht[...], (((1,), (1,)), ((), ())), preferred_element_type=F32
    )
    placed = placed[:MODES] + placed[MODES:]
    for pair in range(g1 // 2):
        a = placed[0:8, pair * LANES : (pair + 1) * LANES]
        b = placed[8:16, pair * LANES : (pair + 1) * LANES]
        s1[2 * pair] = jnp.where(alternate, a, pltpu.roll(b, 4, 1))
        s1[2 * pair + 1] = jnp.where(alternate, pltpu.roll(a, LANES - 4, 1), b)

    def r1_copy(s):
        device, peer = group_peer(s)
        return pltpu.make_async_remote_copy(
            s1.at[peer], r1.at[s], r1_s.at[s], r1_r.at[s], device_id=device, device_id_type=MESH
        )

    def r2_copy(s):
        return pltpu.make_async_remote_copy(
            s2, r2.at[s], r2_s.at[s], r2_r.at[s], device_id=member_peer(s), device_id_type=MESH
        )

    for s in range(1, g1):
        r1_copy(s).start()

    @pl.loop(1, g1, init_carry=s1[group])
    def share(s, total):
        r1_copy(s).wait_recv()
        return total + r1[s]

    s2[...] = share

    for s in range(1, m_count):
        r2_copy(s).start()

    @pl.loop(1, m_count, init_carry=share)
    def final(s, total):
        r2_copy(s).wait_recv()
        return total + r2[s]

    turned = pltpu.roll(final, (LANES - 8 * member) & (LANES - 1), 1)
    turned = turned.T
    charge_ref[...] = jnp.concatenate([turned[0:4], turned[4:8]], 1)

    @pl.loop(1, g1)
    def _(s):
        r1_copy(s).wait_send()

    @pl.loop(1, m_count)
    def _(s):
        r2_copy(s).wait_send()

    for q in range(8):
        @pl.when(exists(q))
        def _(q=q):
            for one in copies(q):
                one.wait_send()

    put.wait()


def local(gx_size, gy_size, charge_density, layer_ids, eps_mean, eps_fluct, galerkin, net_ids, net_place):
    vmem = pl.BlockSpec(memory_space=pltpu.VMEM)
    hbm = pl.BlockSpec(memory_space=pltpu.HBM)
    g1, m_count = SZ * SX, Y_LO * CORES * Y_HI
    tile = (MODES, LANES)
    dma = pltpu.SemaphoreType.DMA
    potential, charges = pl.pallas_call(
        functools.partial(kernel, gx_size, gy_size),
        out_shape=(
            jax.ShapeDtypeStruct((MODES * ROWS, LANES), F32),
            jax.ShapeDtypeStruct((4, MODES), F32),
        ),
        in_specs=[hbm] * 7,
        out_specs=(hbm, vmem),
        scratch_shapes=[
            pltpu.VMEM((MODES * ROWS, LANES), F32),
            pltpu.SemaphoreType.DMA,
            pltpu.VMEM((MODES * ROWS, LANES), F32),
            pltpu.VMEM((ROWS, LANES), I32),
            pltpu.SMEM((LAYERS,), F32),
            pltpu.SMEM((LAYERS, MODES - 1), F32),
            pltpu.VMEM((MODES,) * 3, F32),
            pltpu.VMEM((2, 1, NZ), I32),
            pltpu.VMEM((net_place.shape[0] // LANES, LANES), I32),
            pltpu.SemaphoreType.DMA((7,)),
            pltpu.VMEM((NZ, 2) + tile, F32),
            pltpu.VMEM((ROWS + 4,) + tile, F32),
            pltpu.VMEM((ROWS + 4,) + tile, F32),
            pltpu.VMEM((ROWS,) + tile, F32),
            pltpu.VMEM((ROWS,) + tile, F32),
            pltpu.VMEM((2, NZ) + tile, F32),
            pltpu.VMEM((ROWS,) + tile, F32),
            pltpu.VMEM((ROWS,) + tile, F32),
            pltpu.VMEM((2, ROWS, LANES), I32),
            pltpu.VMEM((3, 1, LANES), I32),
            pltpu.VMEM((8, 3, 1, LANES), I32),
            pltpu.VMEM(tile, F32),
            pltpu.VMEM((2,) + tile, F32),
            pltpu.VMEM((LAYERS * MODES, 3 * MODES), BF16),
            pltpu.VMEM((LAYERS,) + tile, F32),
            pltpu.VMEM((ROWS, LANES), I32),
            pltpu.VMEM((ROWS, LANES), I32),
            pltpu.VMEM((ROWS, LANES), I32),
            pltpu.VMEM((ROWS, LANES), I32),
            pltpu.VMEM((g1 // 2 * LANES, 3 * LANES), BF16),
            pltpu.VMEM((g1, 8, LANES), F32),
            pltpu.VMEM((g1, 8, LANES), F32),
            pltpu.VMEM((8, LANES), F32),
            pltpu.VMEM((m_count, 8, LANES), F32),
            dma((8,)), dma((8,)), dma((2,)), dma((2,)), dma((2,)), dma((2,)), dma((2,)), dma((2,)),
            dma((g1,)), dma((g1,)), dma((m_count,)), dma((m_count,)),
        ],
        compiler_params=pltpu.CompilerParams(
            collective_id=0, has_side_effects=True, vmem_limit_bytes=67043328
        ),
    )(
        charge_density.reshape(MODES * ROWS, LANES),
        layer_ids.reshape(ROWS, LANES),
        eps_mean,
        eps_fluct,
        galerkin,
        jnp.transpose(net_ids, (1, 2, 0)),
        net_place.reshape(-1, LANES),
    )
    return potential.reshape(charge_density.shape), charges.T


def solution(mesh):
    return jax.shard_map(
        functools.partial(local, mesh.shape["gx"], mesh.shape["gy"]),
        mesh=mesh,
        in_specs=(
            P(None, None, "gx", "gy"),
            P(None, "gx", "gy"),
            P(),
            P(),
            P(),
            P(None, "gx", "gy"),
            P(),
        ),
        out_specs=(P(None, None, "gx", "gy"), P(None, ("gx", "gy"))),
        check_vma=False,
    )
```
